512 devices in a mesh: dp: 64 (over y, x, core), mp: 8 (over z).
Axes of the slice: x: 4, y: 8, z: 8, core: 2. Of those that a mesh axis runs over, the one named last changes fastest.
Arguments:
- hidden: bfloat16 [960, 128, 2048], P('dp', None, 'mp'), may hold values from -6 to 6
- attn_out: bfloat16 [960, 128, 2048], P('dp', None, 'mp'), may hold values from -6 to 6
- out_proj: bfloat16 [2048, 2048], P(None, 'mp'), may hold values from -0.125 to 0.125
- norm_gain: float32 [2048], P('mp'), may hold values from 0.1 to 1.9
- reward_proj: float32 [2048, 8], P('mp'), may hold values from -0.125 to 0.125
- block_seq: int32 [960], replicated, may hold values from -1 to 383, as said below
- block_dest: int32 [960], replicated, may hold values from -1 to 639, as said below
- lengths: int32 [384], replicated, may hold values from 1 to 512, as said below
Outputs:
- token_rewards: float32 [640, 8, 128], P('dp')
- advantages: float32 [384], P('dp')
The draws below stay inside these ranges and needn't reach their ends.
Inputs may be any that keep to these rules, and one draw needn't show every extreme that they name: `block_seq`: used slots of each index of dp come first in its 15 slots, the rest hold -1; each index of dp holds 1 to 15 used slots and some index holds exactly 15. Read over used slots in slot order, response numbers never fall, every response appears, and each has 1 to 4 blocks. `block_dest`: exactly the used slots (those of block_seq that are not -1) hold a destination; every owned slot of every owner is named exactly once, so each owner receives exactly 10 blocks; at most 1 block go from one index of dp to one owner, and that many in some pair. `lengths`: A response of n blocks has more than 128 * (n - 1) and at most 128 * n tokens.
All inputs are finite; a program needn't handle non-finite values.
Results may differ from the reference program's by a relative error of at most 0.0029.
Values may be sent and summed in bfloat16 or wider, within the bound.
No kernel may reach another device: no remote copies, remote signals or barrier semaphores. Data moves between devices by JAX's collectives and lax.ppermute only.
A program may use at most 64 MiB of HBM per device.

```python
import jax
import jax.numpy as jnp
from jax import lax

D = 2048
HEADS_R = 8
BLK = 128
MOSTB = 4
OWN_CAP = 10
SLOTS_IN = 15
SEQS = 384
BLOCKS_IN = 960
N_DP = 64


def plan_tables(key):
    base = jax.random.fold_in(key, 4242)
    key_busy, key_cells, key_seqs, key_turn, key_owner, key_length = jax.random.split(base, 6)
    key_longest = jax.random.fold_in(base, 7)
    device_count = BLOCKS_IN // SLOTS_IN
    block_total = OWN_CAP * device_count
    busiest = jax.random.randint(key_busy, (), 0, device_count)
    room_left = SLOTS_IN - 1
    extra_blocks = block_total - (device_count - 1) - SLOTS_IN
    cell_order = jax.random.permutation(key_cells, (device_count - 1) * room_left)
    chosen = (cell_order < extra_blocks).astype(jnp.int32).reshape(device_count - 1, room_left).sum(axis=1)
    positions = jnp.arange(device_count, dtype=jnp.int32)
    shifted = jnp.clip(positions - (positions > busiest).astype(jnp.int32), 0, device_count - 2)
    counts = jnp.where(positions == busiest, SLOTS_IN, 1 + chosen[shifted]).astype(jnp.int32)
    starts = jnp.cumsum(counts) - counts
    slot_pos = jnp.arange(SLOTS_IN, dtype=jnp.int32)
    is_used = (slot_pos[None, :] < counts[:, None]).reshape(-1)
    global_pos = (starts[:, None] + slot_pos[None, :]).reshape(-1)
    global_pos = jnp.where(is_used, global_pos, 0)
    seq_extra = block_total - SEQS
    cell_total = SEQS * (MOSTB - 1)
    longest = jax.random.randint(key_longest, (), 0, SEQS)
    seq_cells = jax.random.permutation(key_seqs, cell_total).astype(jnp.int32)
    cell_index = jnp.arange(cell_total, dtype=jnp.int32)
    cell_row = cell_index // (MOSTB - 1)
    sort_keys = jnp.where(cell_row == longest, -1 - cell_index % (MOSTB - 1), seq_cells)
    cell_rank = jnp.argsort(jnp.argsort(sort_keys, stable=True), stable=True).astype(jnp.int32)
    seq_blocks = 1 + (cell_rank < seq_extra).astype(jnp.int32).reshape(SEQS, MOSTB - 1).sum(axis=1)
    seq_starts = jnp.cumsum(seq_blocks) - seq_blocks
    seq_of = (seq_starts[None, :] <= global_pos[:, None]).astype(jnp.int32).sum(axis=1) - 1
    block_seq = jnp.where(is_used, seq_of, -1)
    rotation = jax.random.randint(key_turn, (), 0, device_count)
    owner_order = jax.random.permutation(key_owner, device_count)
    owner_rank = owner_order[(global_pos + rotation) % device_count]
    destination = jnp.where(is_used, owner_rank * OWN_CAP + global_pos // device_count, -1)
    tail_tokens = jax.random.randint(key_length, (SEQS,), 1, BLK + 1)
    seq_ids = jnp.arange(SEQS, dtype=jnp.int32)
    tail_tokens = jnp.where(seq_ids == longest, BLK, tail_tokens)
    lengths = BLK * (seq_blocks - 1) + tail_tokens
    return (block_seq.astype(jnp.int32), destination.astype(jnp.int32), lengths.astype(jnp.int32))


def draw_block_seq(key, part):
    return plan_tables(key)[0]


def draw_block_dest(key, part):
    return plan_tables(key)[1]


def draw_lengths(key, part):
    return plan_tables(key)[2]


def shard_levels(key, dims, shards, least, largest):
    loudness, own = 1.0, jax.random.fold_in(key, 6)
    for axis_at, shards_of in shards:
        heights = jnp.exp(jax.random.uniform(jax.random.fold_in(own, axis_at), (shards_of,), jnp.float32, least / len(shards), largest / len(shards)))
        loudness = loudness * jnp.repeat(heights, dims[axis_at] // shards_of).reshape([-1 if axis == axis_at else 1 for axis in range(len(dims))])
    return loudness


def centred(rng, dims, scale, reach, pieces=(), kind=jnp.bfloat16):
    loudness = shard_levels(rng, dims, pieces, -0.22, 0.18) if pieces else 1.0
    entries = jax.random.normal(rng, dims, jnp.float32) * scale * loudness
    return jnp.minimum(jnp.maximum(entries, -reach), reach).astype(kind)


def setup_inputs(seed: int = 0) -> dict:
    arg_keys = jax.random.split(jax.random.key(seed), 9)
    return {
        "hidden": centred(arg_keys[0], (BLOCKS_IN, BLK, D), 1.0, 6.0, ((0, 64), (2, 8))),
        "attn_out": centred(arg_keys[1], (BLOCKS_IN, BLK, D), 1.0, 6.0, ((0, 64), (2, 8))),
        "out_proj": centred(arg_keys[2], (D, D), D ** -0.5, 0.125, ((1, 8),)),
        "norm_gain": jnp.clip(1.0 + 0.18 * jax.random.normal(arg_keys[3], (D,), jnp.float32), 0.1, 1.9),
        "reward_proj": centred(arg_keys[4], (D, HEADS_R), D ** -0.5, 0.125, ((0, 8),), jnp.float32),
        "block_seq": draw_block_seq(jax.random.fold_in(arg_keys[8], 71), 0),
        "block_dest": draw_block_dest(jax.random.fold_in(arg_keys[8], 71), 0),
        "lengths": draw_lengths(jax.random.fold_in(arg_keys[8], 71), 0),
    }


norm_epsilon = 1e-05
stat_epsilon = 1e-06

def reference(hidden, attn_out, out_proj, norm_gain, reward_proj, block_seq, block_dest, lengths):
    slot_count = block_seq.shape[0]
    owned_count = OWN_CAP * N_DP
    slot_index = jnp.arange(slot_count, dtype=jnp.int32)
    is_used = block_dest >= 0
    target = jnp.where(is_used, block_dest, owned_count).astype(jnp.int32)
    source = jnp.zeros((owned_count,), jnp.int32).at[target].set(slot_index, mode='drop')
    seq_safe = jnp.where(is_used, block_seq, 0).astype(jnp.int32)
    used_int = is_used.astype(jnp.int32)
    per_seq = jnp.zeros((SEQS,), jnp.int32).at[seq_safe].add(used_int)
    seq_starts = jnp.cumsum(per_seq) - per_seq
    global_pos = jnp.cumsum(used_int) - 1
    seq_rank = global_pos - seq_starts[seq_safe]
    valid_tokens = jnp.minimum(BLK, lengths[seq_safe] - BLK * seq_rank)
    src_seq = seq_safe[source]
    src_valid = valid_tokens[source]

    def one_block(slot):
        projected = jnp.dot(attn_out[slot], out_proj, preferred_element_type=jnp.float32)
        stored = (hidden[slot].astype(jnp.float32) + projected).astype(jnp.bfloat16)
        stored = lax.optimization_barrier(stored)
        values = stored.astype(jnp.float32)
        mean_sq = lax.optimization_barrier(jnp.mean(values * values, axis=1, keepdims=True))
        normed = values * lax.rsqrt(mean_sq + norm_epsilon) * norm_gain[None, :]
        return jnp.dot(normed, reward_proj, precision=lax.Precision.HIGHEST)
    rewards = lax.map(one_block, source)
    live = jnp.arange(BLK, dtype=jnp.int32)[None, :] < src_valid[:, None]
    rewards = jnp.where(live[:, :, None], rewards, jnp.float32(0.0))
    token_rewards = jnp.transpose(rewards, (0, 2, 1))
    block_sums = lax.optimization_barrier(jnp.sum(token_rewards, axis=2))
    seq_totals = jnp.zeros((SEQS, HEADS_R), jnp.float32).at[src_seq].add(block_sums)
    scores = seq_totals / lengths[:, None].astype(jnp.float32)
    worst_case = lax.optimization_barrier(jnp.min(scores, axis=1))
    head_mean = lax.optimization_barrier(jnp.mean(scores, axis=1))
    spread = lax.optimization_barrier(jnp.mean((scores - head_mean[:, None]) ** 2, axis=1))
    penalty_scale = jnp.mean(spread) + stat_epsilon
    conservative = worst_case - spread / penalty_scale
    centre = jnp.mean(conservative)
    variance = jnp.mean((conservative - centre) ** 2)
    advantages = (conservative - centre) / jnp.sqrt(variance + stat_epsilon)
    return (token_rewards, advantages)
```

```python
import jax
import jax.numpy as jnp
from jax import lax
from jax.experimental import pallas as pl
from jax.experimental.pallas import tpu as pltpu
from jax.sharding import Mesh
from jax.sharding import PartitionSpec as P

OWN_CAP = 10
NORM_EPS = 1e-05
STAT_EPS = 1e-06
F32 = jnp.float32
BF16 = jnp.bfloat16
ROWS = 128
PLANES = 8
TOK = 16


def exchange(value, axis):
    return lax.all_to_all(value, axis, split_axis=0, concat_axis=0, tiled=True)


def shift(value, axis, step):
    size = lax.axis_size(axis)
    return lax.ppermute(value, axis, [(s, (s + step) % size) for s in range(size)])


def swap(value, axis):
    size = lax.axis_size(axis)
    return lax.ppermute(value, axis, [(s, s ^ 1) for s in range(size)])


def score_kernel(
    where_ref, acts_ref, q_ref, r1_ref, r3_ref, f1_ref, f3_ref,
    qo_ref, r1o_ref, r3o_ref, f1o_ref, f3o_ref, wt_ref, live_ref, route_ref,
    out_ref, a_ref, sq_ref, head_ref,
):
    tokens = live_ref.shape[0]
    core = where_ref[8]
    own_at = pl.multiple_of(core * ROWS, ROWS)
    other_at = pl.multiple_of((1 - core) * ROWS, ROWS)
    for s in range(8):
        i = where_ref[s]
        a_ref[:, 2 * s * ROWS : (2 * s + 1) * ROWS] = acts_ref[i, 0:tokens, pl.ds(own_at, ROWS)]
        a_ref[:, (2 * s + 1) * ROWS : (2 * s + 2) * ROWS] = acts_ref[i, 0:tokens, pl.ds(other_at, ROWS)]
    for j in range(PLANES):
        weights = jnp.concatenate(
            [
                q_ref[0, j], qo_ref[0, j], q_ref[1, j], qo_ref[1, j],
                r1_ref[0, j], r1o_ref[0, j], r1_ref[1, j], r1o_ref[1, j],
                r3_ref[0, j], r3o_ref[0, j], r3_ref[1, j], r3o_ref[1, j],
                f1_ref[j], f1o_ref[j], f3_ref[j], f3o_ref[j],
            ],
            axis=0,
        )
        proj = jnp.dot(a_ref[...], weights, preferred_element_type=F32)
        resid = (acts_ref[j, tokens : 2 * tokens, :].astype(F32) + proj).astype(BF16)
        value = resid.astype(F32)
        heads = lax.dot_general(
            resid, wt_ref[j], (((1,), (1,)), ((), ())), preferred_element_type=F32
        )
        if j == 0:
            sq_ref[...] = value * value
            head_ref[...] = heads
        else:
            sq_ref[...] += value * value
            head_ref[...] += heads
    width = float(PLANES * acts_ref.shape[2])
    mean_sq = jnp.sum(sq_ref[...], axis=1, keepdims=True) / width
    scale = lax.rsqrt(mean_sq + NORM_EPS) * live_ref[...]
    k = lax.broadcasted_iota(jnp.int32, (16, 128), 0)
    lane = lax.broadcasted_iota(jnp.int32, (16, 128), 1)
    spread_heads = (k % 8 == lane // TOK).astype(F32)
    wide = jnp.dot(
        head_ref[...], spread_heads, precision=lax.Precision.HIGHEST, preferred_element_type=F32
    )
    wide = wide * scale
    row = lax.broadcasted_iota(jnp.int32, (tokens, 128), 0)
    col = lax.broadcasted_iota(jnp.int32, (tokens, 128), 1)
    by_token = jnp.where(row % TOK == col % TOK, wide, 0.0)
    by_slot = jnp.where(row // TOK == col % TOK, wide, 0.0)
    out_ref[:, 0, :] = jnp.dot(
        route_ref[...], by_token, precision=lax.Precision.HIGHEST, preferred_element_type=F32
    )
    out_ref[:, 1, :] = jnp.broadcast_to(
        jnp.sum(by_slot, axis=0, keepdims=True), (out_ref.shape[0], 128)
    )


def score(*args):
    owners = args[-1].shape[0]
    tokens = args[-2].shape[0]
    width = PLANES * args[1].shape[2]
    vmem = pl.BlockSpec(memory_space=pltpu.VMEM)
    return pl.pallas_call(
        score_kernel,
        out_shape=jax.ShapeDtypeStruct((owners, 2, 128), F32),
        in_specs=[pl.BlockSpec(memory_space=pltpu.SMEM)] + [vmem] * (len(args) - 1),
        out_specs=vmem,
        scratch_shapes=[
            pltpu.VMEM((tokens, width), BF16),
            pltpu.VMEM((tokens, args[1].shape[2]), F32),
            pltpu.VMEM((tokens, 16), F32),
        ],
        name="score",
    )(*args)


def local(hidden, attn_out, out_proj, norm_gain, reward_proj, block_seq, block_dest, lengths):
    y, x, core, plane = (lax.axis_index(n) for n in ("y", "x", "core", "mp"))
    rank = (y * lax.axis_size("x") + x) * 2 + core
    owners = 64
    slots_in, block_len, shard = hidden.shape
    seq_count = lengths.shape[0]
    seq_local = seq_count // owners
    tokens = slots_in * TOK

    parity = y % 2
    piece = lax.dynamic_slice_in_dim(out_proj, x * 4 * ROWS + parity * 2 * ROWS + core * ROWS, ROWS, 0)
    weighted = (norm_gain[:, None] * reward_proj).T
    high = lax.reduce_precision(weighted, 8, 7)
    low = weighted - high
    piece = jnp.concatenate([piece, high.astype(BF16), low.astype(BF16)], axis=0)
    planes = exchange(jnp.broadcast_to(piece[None], (PLANES, *piece.shape)), "mp")
    head_rows = planes[:, ROWS:, :]
    first = planes[:, :ROWS, :]

    both = [v.reshape(slots_in, PLANES, TOK, shard).swapaxes(0, 1).reshape(PLANES, tokens, shard) for v in (attn_out, hidden)]
    acts = jnp.concatenate(both, axis=1)
    acts, first = lax.optimization_barrier((acts, first))
    acts = exchange(acts, "mp")

    q = jnp.stack([first, swap(first, "y")])
    r1, r3 = shift(q, "x", 1), shift(q, "x", -1)
    f1, f3 = shift(r1[0], "x", 1), shift(r3[1], "x", -1)
    pieces = (q, r1, r3, f1, f3)
    others = tuple(swap(v, "core") for v in pieces)
    xs = jnp.stack([x, x, (x + 3) % 4, (x + 3) % 4, (x + 1) % 4, (x + 1) % 4, (x + 2) % 4, (x + 2) % 4])
    odd = jnp.arange(8, dtype=jnp.int32) % 2
    where = jnp.concatenate([2 * xs + (parity ^ odd), core[None]]).astype(jnp.int32)

    all_slots = jnp.arange(block_seq.shape[0], dtype=jnp.int32)
    mine = rank * slots_in + jnp.arange(slots_in, dtype=jnp.int32)
    seq_in = lax.dynamic_slice_in_dim(block_seq, rank * slots_in, slots_in)
    dest_in = lax.dynamic_slice_in_dim(block_dest, rank * slots_in, slots_in)
    earlier = (block_seq[None, :] == seq_in[:, None]) & (all_slots[None, :] < mine[:, None])
    order = jnp.sum(earlier.astype(jnp.int32), axis=1)
    seq_ids = jnp.arange(seq_count, dtype=jnp.int32)
    length_in = jnp.sum(jnp.where(seq_ids[None, :] == seq_in[:, None], lengths[None, :], 0), axis=1)
    valid = jnp.where(dest_in >= 0, jnp.minimum(block_len, length_in - block_len * order), 0)
    at = plane * TOK + jnp.arange(TOK, dtype=jnp.int32)
    live = (at[None, :] < valid[:, None]).astype(F32).reshape(tokens, 1)
    owner_in = jnp.where(dest_in >= 0, dest_in // OWN_CAP, -1)
    owner_of = jnp.broadcast_to(owner_in[:, None], (slots_in, TOK)).reshape(1, tokens)
    route = (jnp.arange(owners, dtype=jnp.int32)[:, None] == owner_of).astype(F32)

    sent = score(where, acts, *pieces, *others, head_rows, live, route)
    got = exchange(sent, ("y", "x", "core"))

    targets = rank * OWN_CAP + jnp.arange(OWN_CAP, dtype=jnp.int32)
    source = jnp.sum(jnp.where(block_dest[None, :] == targets[:, None], all_slots[None, :], 0), axis=1)
    pick = ((source // slots_in)[:, None] == jnp.arange(owners, dtype=jnp.int32)[None, :]).astype(F32)
    member = (block_seq[:, None] == seq_ids[None, :]).astype(F32)

    owned = jnp.dot(pick, got[:, 0, :], precision=lax.Precision.HIGHEST)
    sums = got[:, 1, :].reshape(owners, 8, TOK)[:, :, :slots_in].swapaxes(0, 1).reshape(8, owners * slots_in)
    totals = jnp.dot(sums, member, precision=lax.Precision.HIGHEST)
    final = jnp.concatenate([owned, totals.reshape(-1, 128)], axis=0)
    final = exchange(jnp.broadcast_to(final[None], (PLANES, *final.shape)), "mp")
    token_rewards = (
        final[:, :OWN_CAP].reshape(PLANES, OWN_CAP, 8, TOK).transpose(1, 2, 0, 3).reshape(OWN_CAP, 8, block_len)
    )
    totals = jnp.sum(final[:, OWN_CAP:], axis=0).reshape(8, seq_count)
    scores = totals / lengths.astype(F32)[None, :]
    worst = jnp.min(scores, axis=0)
    head_mean = jnp.mean(scores, axis=0)
    spread = jnp.mean((scores - head_mean[None, :]) ** 2, axis=0)
    penalty_scale = jnp.mean(spread) + STAT_EPS
    conservative = worst - spread / penalty_scale
    centre = jnp.mean(conservative)
    variance = jnp.mean((conservative - centre) ** 2)
    advantages = (conservative - centre) / jnp.sqrt(variance + STAT_EPS)
    return token_rewards, lax.dynamic_slice_in_dim(advantages, rank * seq_local, seq_local)


def solution(mesh):
    dp = ("y", "x", "core")
    grid = Mesh(mesh.devices.reshape(8, 4, 2, PLANES), (*dp, "mp"))
    return jax.shard_map(
        local,
        mesh=grid,
        in_specs=(
            P(dp, None, "mp"),
            P(dp, None, "mp"),
            P(None, "mp"),
            P("mp"),
            P("mp", None),
            P(),
            P(),
            P(),
        ),
        out_specs=(P(dp, None, None), P(dp)),
        check_vma=False,
    )
```

```python
import jax
import jax.numpy as jnp
from jax import lax
from jax.experimental import pallas as pl
from jax.experimental.pallas import tpu as pltpu
from jax.sharding import Mesh
from jax.sharding import PartitionSpec as P

OWN_CAP = 10
NORM_EPS = 1e-05
STAT_EPS = 1e-06
F32 = jnp.float32
BF16 = jnp.bfloat16
ROWS = 128
PLANES = 8
TOK = 16


def exchange(value, axis):
    return lax.all_to_all(value, axis, split_axis=0, concat_axis=0, tiled=True)


def shift(value, axis, step):
    size = lax.axis_size(axis)
    return lax.ppermute(value, axis, [(s, (s + step) % size) for s in range(size)])


def swap(value, axis):
    size = lax.axis_size(axis)
    return lax.ppermute(value, axis, [(s, s ^ 1) for s in range(size)])


def score_kernel(
    where_ref, acts_ref, *refs,
):
    pieces = refs[:16]
    live_ref, route_ref, out_ref, a_ref, w_ref, sq_ref, head_ref, sem = refs[16:]
    tokens = live_ref.shape[0]

    def fetch(j, p):
        return pltpu.make_async_copy(
            pieces[p].at[j], w_ref.at[j, pl.ds(p * ROWS, ROWS)], sem.at[j, p]
        )

    for j in range(PLANES):
        for p in range(16):
            fetch(j, p).start()
    core = where_ref[8]
    own_at = pl.multiple_of(core * ROWS, ROWS)
    other_at = pl.multiple_of((1 - core) * ROWS, ROWS)
    for s in range(8):
        i = where_ref[s]
        a_ref[:, 2 * s * ROWS : (2 * s + 1) * ROWS] = acts_ref[i, 0:tokens, pl.ds(own_at, ROWS)]
        a_ref[:, (2 * s + 1) * ROWS : (2 * s + 2) * ROWS] = acts_ref[i, 0:tokens, pl.ds(other_at, ROWS)]
    for j in range(PLANES):
        for p in range(16):
            fetch(j, p).wait()
        proj = jnp.dot(a_ref[...], w_ref[j], preferred_element_type=F32)
        resid = (acts_ref[j, tokens : 2 * tokens, :].astype(F32) + proj).astype(BF16)
        value = resid.astype(F32)
        heads = lax.dot_general(
            resid, acts_ref[j, 2 * tokens :, :], (((1,), (1,)), ((), ())), preferred_element_type=F32
        )
        if j == 0:
            sq_ref[...] = value * value
            head_ref[...] = heads
        else:
            sq_ref[...] += value * value
            head_ref[...] += heads
    width = float(PLANES * acts_ref.shape[2])
    mean_sq = jnp.sum(sq_ref[...], axis=1, keepdims=True) / width
    scale = lax.rsqrt(mean_sq + NORM_EPS) * live_ref[...]
    k = lax.broadcasted_iota(jnp.int32, (16, 128), 0)
    lane = lax.broadcasted_iota(jnp.int32, (16, 128), 1)
    spread_heads = (k % 8 == lane // TOK).astype(F32)
    wide = jnp.dot(
        head_ref[...], spread_heads, precision=lax.Precision.HIGHEST, preferred_element_type=F32
    )
    wide = wide * scale
    row = lax.broadcasted_iota(jnp.int32, (tokens, 128), 0)
    col = lax.broadcasted_iota(jnp.int32, (tokens, 128), 1)
    by_token = jnp.where(row % TOK == col % TOK, wide, 0.0)
    by_slot = jnp.where(row // TOK == col % TOK, wide, 0.0)
    out_ref[:, 0, :] = jnp.dot(
        route_ref[...], by_token, precision=lax.Precision.HIGHEST, preferred_element_type=F32
    )
    out_ref[:, 1, :] = jnp.broadcast_to(
        jnp.sum(by_slot, axis=0, keepdims=True), (out_ref.shape[0], 128)
    )


def in_vmem(value):
    return pltpu.with_memory_space_constraint(value, pltpu.VMEM)


def score(where, *args):
    owners = args[-1].shape[0]
    tokens = args[-2].shape[0]
    width = PLANES * args[0].shape[2]
    vmem = pl.BlockSpec(memory_space=pltpu.VMEM)
    return pl.pallas_call(
        score_kernel,
        out_shape=jax.ShapeDtypeStruct((owners, 2, 128), F32),
        in_specs=[
            pl.BlockSpec(memory_space=pltpu.SMEM),
            vmem,
            *[pl.BlockSpec(memory_space=pl.ANY)] * 16,
            vmem,
            vmem,
        ],
        out_specs=vmem,
        scratch_shapes=[
            pltpu.VMEM((tokens, width), BF16),
            pltpu.VMEM((PLANES, width, args[0].shape[2]), BF16),
            pltpu.VMEM((tokens, args[0].shape[2]), F32),
            pltpu.VMEM((tokens, 16), F32),
            pltpu.SemaphoreType.DMA((PLANES, 16)),
        ],
        compiler_params=pltpu.CompilerParams(vmem_limit_bytes=24 * 2**20),
        name="score",
    )(where, in_vmem(args[0]), *[pltpu.with_memory_space_constraint(v, pltpu.HBM) for v in args[1:17]], *args[17:])


def finish_kernel(totals_ref, lengths_ref, rank_ref, out_ref):
    totals = totals_ref[0]
    for p in range(1, PLANES):
        totals = totals + totals_ref[p]
    scores = totals / lengths_ref[...].astype(F32)
    count = float(scores.shape[1])
    worst = jnp.min(scores, axis=0, keepdims=True)
    head_mean = jnp.mean(scores, axis=0, keepdims=True)
    spread = jnp.mean((scores - head_mean) ** 2, axis=0, keepdims=True)
    penalty_scale = jnp.sum(spread, axis=1, keepdims=True) / count + STAT_EPS
    conservative = worst - spread / penalty_scale
    centre = jnp.sum(conservative, axis=1, keepdims=True) / count
    off = conservative - centre
    variance = jnp.sum(off * off, axis=1, keepdims=True) / count
    advantages = off / jnp.sqrt(variance + STAT_EPS)
    size = out_ref.shape[0]
    at = lax.broadcasted_iota(jnp.int32, (size, scores.shape[1]), 1)
    row = lax.broadcasted_iota(jnp.int32, (size, scores.shape[1]), 0)
    mine = jnp.where(at == row + rank_ref[0] * size, advantages, 0.0)
    out_ref[...] = jnp.sum(mine, axis=1, keepdims=True)


def finish(totals, lengths, rank, size):
    vmem = pl.BlockSpec(memory_space=pltpu.VMEM)
    return pl.pallas_call(
        finish_kernel,
        out_shape=jax.ShapeDtypeStruct((size, 1), F32),
        in_specs=[vmem, vmem, pl.BlockSpec(memory_space=pltpu.SMEM)],
        out_specs=vmem,
        compiler_params=pltpu.CompilerParams(vmem_limit_bytes=8 * 2**20),
        name="finish",
    )(in_vmem(totals), lengths[None, :], rank[None])


def local(hidden, attn_out, out_proj, norm_gain, reward_proj, block_seq, block_dest, lengths):
    y, x, core, plane = (lax.axis_index(n) for n in ("y", "x", "core", "mp"))
    rank = (y * lax.axis_size("x") + x) * 2 + core
    owners = 64
    slots_in, block_len, shard = hidden.shape
    seq_count = lengths.shape[0]
    seq_local = seq_count // owners
    tokens = slots_in * TOK

    parity = y % 2
    piece = lax.dynamic_slice_in_dim(out_proj, x * 4 * ROWS + parity * 2 * ROWS + core * ROWS, ROWS, 0)
    first = exchange(jnp.broadcast_to(piece[None], (PLANES, *piece.shape)), "mp")

    weighted = (norm_gain[:, None] * reward_proj).T
    high = lax.reduce_precision(weighted, 8, 7)
    low = weighted - high
    head_rows = jnp.concatenate([high.astype(BF16), low.astype(BF16)], axis=0)
    sliced = [
        v.reshape(slots_in, PLANES, TOK, shard).swapaxes(0, 1).reshape(PLANES, tokens, shard)
        for v in (attn_out, hidden)
    ]
    acts = jnp.concatenate([*sliced, jnp.broadcast_to(head_rows[None], (PLANES, *head_rows.shape))], axis=1)
    acts, first = lax.optimization_barrier((acts, first))
    acts = exchange(acts, "mp")

    second = swap(first, "y")
    left = [shift(first, "x", 1), shift(second, "x", 1)]
    right = [shift(first, "x", -1), shift(second, "x", -1)]
    far = [shift(left[0], "x", 1), shift(right[1], "x", -1)]
    pieces = [first, second, *left, *right, *far]
    pieces = [v for own in pieces for v in (own, swap(own, "core"))]
    xs = jnp.stack([x, x, (x + 3) % 4, (x + 3) % 4, (x + 1) % 4, (x + 1) % 4, (x + 2) % 4, (x + 2) % 4])
    odd = jnp.arange(8, dtype=jnp.int32) % 2
    where = jnp.concatenate([2 * xs + (parity ^ odd), core[None]]).astype(jnp.int32)

    all_slots = jnp.arange(block_seq.shape[0], dtype=jnp.int32)
    mine = rank * slots_in + jnp.arange(slots_in, dtype=jnp.int32)
    seq_in = lax.dynamic_slice_in_dim(block_seq, rank * slots_in, slots_in)
    dest_in = lax.dynamic_slice_in_dim(block_dest, rank * slots_in, slots_in)
    earlier = (block_seq[None, :] == seq_in[:, None]) & (all_slots[None, :] < mine[:, None])
    order = jnp.sum(earlier.astype(jnp.int32), axis=1)
    seq_ids = jnp.arange(seq_count, dtype=jnp.int32)
    length_in = jnp.sum(jnp.where(seq_ids[None, :] == seq_in[:, None], lengths[None, :], 0), axis=1)
    valid = jnp.where(dest_in >= 0, jnp.minimum(block_len, length_in - block_len * order), 0)
    at = plane * TOK + jnp.arange(TOK, dtype=jnp.int32)
    live = (at[None, :] < valid[:, None]).astype(F32).reshape(tokens, 1)
    owner_in = jnp.where(dest_in >= 0, dest_in // OWN_CAP, -1)
    owner_of = jnp.broadcast_to(owner_in[:, None], (slots_in, TOK)).reshape(1, tokens)
    route = (jnp.arange(owners, dtype=jnp.int32)[:, None] == owner_of).astype(F32)

    sent = score(where, acts, *pieces, live, route)
    got = exchange(sent, ("y", "x", "core"))

    targets = rank * OWN_CAP + jnp.arange(OWN_CAP, dtype=jnp.int32)
    source = jnp.sum(jnp.where(block_dest[None, :] == targets[:, None], all_slots[None, :], 0), axis=1)
    pick = ((source // slots_in)[:, None] == jnp.arange(owners, dtype=jnp.int32)[None, :]).astype(F32)
    member = (block_seq[:, None] == seq_ids[None, :]).astype(F32)

    owned = jnp.dot(pick, got[:, 0, :], precision=lax.Precision.HIGHEST)
    sums = got[:, 1, :].reshape(owners, 8, TOK)[:, :, :slots_in].swapaxes(0, 1).reshape(8, owners * slots_in)
    totals = jnp.dot(sums, member, precision=lax.Precision.HIGHEST)
    final = jnp.concatenate([owned, totals.reshape(-1, 128)], axis=0)
    final = exchange(jnp.broadcast_to(final[None], (PLANES, *final.shape)), "mp")
    token_rewards = (
        final[:, :OWN_CAP].reshape(PLANES, OWN_CAP, 8, TOK).transpose(1, 2, 0, 3).reshape(OWN_CAP, 8, block_len)
    )
    totals = final[:, OWN_CAP:].reshape(PLANES, 8, seq_count)
    return token_rewards, finish(totals, lengths, rank, seq_local).reshape(seq_local)


def solution(mesh):
    dp = ("y", "x", "core")
    grid = Mesh(mesh.devices.reshape(8, 4, 2, PLANES), (*dp, "mp"))
    return jax.shard_map(
        local,
        mesh=grid,
        in_specs=(
            P(dp, None, "mp"),
            P(dp, None, "mp"),
            P(None, "mp"),
            P("mp"),
            P("mp", None),
            P(),
            P(),
            P(),
        ),
        out_specs=(P(dp, None, None), P(dp)),
        check_vma=False,
    )
```

```python
import jax
import jax.numpy as jnp
from jax import lax
from jax.experimental import pallas as pl
from jax.experimental.pallas import tpu as pltpu
from jax.sharding import Mesh
from jax.sharding import PartitionSpec as P

OWN_CAP = 10
NORM_EPS = 1e-05
STAT_EPS = 1e-06
F32 = jnp.float32
BF16 = jnp.bfloat16
PLANES = 8
TOK = 16


def exchange(value, axis):
    return lax.all_to_all(value, axis, split_axis=0, concat_axis=0, tiled=True)


def shift(value, axis, step):
    size = lax.axis_size(axis)
    return lax.ppermute(value, axis, [(s, (s + step) % size) for s in range(size)])


def swap(value, axis):
    size = lax.axis_size(axis)
    return lax.ppermute(value, axis, [(s, s ^ 1) for s in range(size)])


def plane_step(kind, part):
    return (kind if part % 2 == 0 else PLANES - kind) + 4 * (part // 2)


def from_plane(value, part):
    pairs = []
    for y in range(8):
        for x in range(4):
            step = plane_step((y % 2) * 4 + x, part)
            for core in range(2):
                base = ((y * 4 + x) * 2 + core) * PLANES
                pairs += [(base + (z + step) % PLANES, base + z) for z in range(PLANES)]
    return lax.ppermute(value, ("y", "x", "core", "mp"), pairs)


def score_kernel(where_ref, acts_ref, *refs):
    pieces = refs[:16]
    live_ref, route_ref, out_ref, a_ref, w_ref, sq_ref, head_ref, sem = refs[16:]
    tokens = live_ref.shape[0]
    shard = acts_ref.shape[2]
    core = where_ref[32]

    def fetch(s, p):
        row = 2 * p + (core if s % 2 == 0 else 1 - core)
        return pltpu.make_async_copy(
            pieces[s].at[p], w_ref.at[where_ref[(s // 2) * 4 + p], row], sem.at[s, p]
        )

    for s in range(16):
        for p in range(4):
            fetch(s, p).start()
    for i in range(PLANES):
        a_ref[:, i * shard : (i + 1) * shard] = acts_ref[i, 0:tokens, :]
    for s in range(16):
        for p in range(4):
            fetch(s, p).wait()
    for j in range(PLANES):
        weights = w_ref[j].reshape(PLANES * shard, shard)
        proj = jnp.dot(a_ref[...], weights, preferred_element_type=F32)
        resid = (acts_ref[j, tokens : 2 * tokens, :].astype(F32) + proj).astype(BF16)
        value = resid.astype(F32)
        heads = lax.dot_general(
            resid, acts_ref[j, 2 * tokens :, :], (((1,), (1,)), ((), ())), preferred_element_type=F32
        )
        if j == 0:
            sq_ref[...] = value * value
            head_ref[...] = heads
        else:
            sq_ref[...] += value * value
            head_ref[...] += heads
    width = float(PLANES * acts_ref.shape[2])
    mean_sq = jnp.sum(sq_ref[...], axis=1, keepdims=True) / width
    scale = lax.rsqrt(mean_sq + NORM_EPS) * live_ref[...]
    k = lax.broadcasted_iota(jnp.int32, (16, 128), 0)
    lane = lax.broadcasted_iota(jnp.int32, (16, 128), 1)
    spread_heads = (k % 8 == lane // TOK).astype(F32)
    wide = jnp.dot(
        head_ref[...], spread_heads, precision=lax.Precision.HIGHEST, preferred_element_type=F32
    )
    wide = wide * scale
    row = lax.broadcasted_iota(jnp.int32, (tokens, 128), 0)
    col = lax.broadcasted_iota(jnp.int32, (tokens, 128), 1)
    by_token = jnp.where(row % TOK == col % TOK, wide, 0.0)
    by_slot = jnp.where(row // TOK == col % TOK, wide, 0.0)
    out_ref[:, 0, :] = jnp.dot(
        route_ref[...], by_token, precision=lax.Precision.HIGHEST, preferred_element_type=F32
    )
    out_ref[:, 1, :] = jnp.broadcast_to(
        jnp.sum(by_slot, axis=0, keepdims=True), (out_ref.shape[0], 128)
    )


def in_vmem(value):
    return pltpu.with_memory_space_constraint(value, pltpu.VMEM)


def score(where, *args):
    owners = args[-1].shape[0]
    tokens = args[-2].shape[0]
    width = PLANES * args[0].shape[2]
    vmem = pl.BlockSpec(memory_space=pltpu.VMEM)
    return pl.pallas_call(
        score_kernel,
        out_shape=jax.ShapeDtypeStruct((owners, 2, 128), F32),
        in_specs=[
            pl.BlockSpec(memory_space=pltpu.SMEM),
            vmem,
            *[pl.BlockSpec(memory_space=pl.ANY)] * 16,
            vmem,
            vmem,
        ],
        out_specs=vmem,
        scratch_shapes=[
            pltpu.VMEM((tokens, width), BF16),
            pltpu.VMEM((PLANES, PLANES, args[0].shape[2], args[0].shape[2]), BF16),
            pltpu.VMEM((tokens, args[0].shape[2]), F32),
            pltpu.VMEM((tokens, 16), F32),
            pltpu.SemaphoreType.DMA((16, 4)),
        ],
        compiler_params=pltpu.CompilerParams(vmem_limit_bytes=24 * 2**20),
        name="score",
    )(where, in_vmem(args[0]), *[pltpu.with_memory_space_constraint(v, pltpu.HBM) for v in args[1:17]], *args[17:])


def finish_kernel(totals_ref, lengths_ref, rank_ref, out_ref):
    totals = totals_ref[0]
    for p in range(1, PLANES):
        totals = totals + totals_ref[p]
    scores = totals / lengths_ref[...].astype(F32)
    count = float(scores.shape[1])
    worst = jnp.min(scores, axis=0, keepdims=True)
    head_mean = jnp.mean(scores, axis=0, keepdims=True)
    spread = jnp.mean((scores - head_mean) ** 2, axis=0, keepdims=True)
    penalty_scale = jnp.sum(spread, axis=1, keepdims=True) / count + STAT_EPS
    conservative = worst - spread / penalty_scale
    centre = jnp.sum(conservative, axis=1, keepdims=True) / count
    off = conservative - centre
    variance = jnp.sum(off * off, axis=1, keepdims=True) / count
    advantages = off / jnp.sqrt(variance + STAT_EPS)
    size = out_ref.shape[0]
    at = lax.broadcasted_iota(jnp.int32, (size, scores.shape[1]), 1)
    row = lax.broadcasted_iota(jnp.int32, (size, scores.shape[1]), 0)
    mine = jnp.where(at == row + rank_ref[0] * size, advantages, 0.0)
    out_ref[...] = jnp.sum(mine, axis=1, keepdims=True)


def finish(totals, lengths, rank, size):
    vmem = pl.BlockSpec(memory_space=pltpu.VMEM)
    return pl.pallas_call(
        finish_kernel,
        out_shape=jax.ShapeDtypeStruct((size, 1), F32),
        in_specs=[vmem, vmem, pl.BlockSpec(memory_space=pltpu.SMEM)],
        out_specs=vmem,
        compiler_params=pltpu.CompilerParams(vmem_limit_bytes=8 * 2**20),
        name="finish",
    )(in_vmem(totals), lengths[None, :], rank[None])


def local(hidden, attn_out, out_proj, norm_gain, reward_proj, block_seq, block_dest, lengths):
    y, x, core, plane = (lax.axis_index(n) for n in ("y", "x", "core", "mp"))
    rank = (y * lax.axis_size("x") + x) * 2 + core
    owners = 64
    slots_in, block_len, shard = hidden.shape
    seq_count = lengths.shape[0]
    seq_local = seq_count // owners
    tokens = slots_in * TOK

    parity = y % 2
    blocks = out_proj.reshape(4, 2, shard, shard)
    parts = []
    for p in range(4):
        block = lax.dynamic_index_in_dim(blocks[p], core, 0, keepdims=False)
        parts.append(from_plane(block, p))
    first = jnp.stack(parts)

    weighted = (norm_gain[:, None] * reward_proj).T
    high = lax.reduce_precision(weighted, 8, 7)
    low = weighted - high
    head_rows = jnp.concatenate([high.astype(BF16), low.astype(BF16)], axis=0)
    sliced = [
        v.reshape(slots_in, PLANES, TOK, shard).swapaxes(0, 1).reshape(PLANES, tokens, shard)
        for v in (attn_out, hidden)
    ]
    acts = jnp.concatenate([*sliced, jnp.broadcast_to(head_rows[None], (PLANES, *head_rows.shape))], axis=1)
    acts = exchange(acts, "mp")

    second = swap(first, "y")
    left0 = shift(first, "x", 1)
    right0 = shift(first, "x", -1)
    left1 = shift(second, "x", 1)
    right1 = shift(second, "x", -1)
    far0 = shift(left0, "x", 1)
    far1 = shift(right1, "x", -1)
    named = {
        "c0": first, "c1": second, "cl0": left0, "cl1": left1,
        "cr0": right0, "cr1": right1, "cf0": far0, "cf1": far1,
    }
    pieces = []
    for own in named.values():
        pieces += [own, swap(own, "core")]
    odd = jnp.array([0, 1, 0, 1, 0, 1, 0, 1], jnp.int32)
    away = jnp.array([0, 0, 3, 3, 1, 1, 2, 2], jnp.int32)
    kind = (parity ^ odd) * 4 + (x + away) % 4
    held = [(plane + plane_step(kind, p)) % PLANES for p in range(4)]
    where = jnp.concatenate([jnp.stack(held, axis=1).reshape(32), core[None]]).astype(jnp.int32)

    all_slots = jnp.arange(block_seq.shape[0], dtype=jnp.int32)
    mine = rank * slots_in + jnp.arange(slots_in, dtype=jnp.int32)
    seq_in = lax.dynamic_slice_in_dim(block_seq, rank * slots_in, slots_in)
    dest_in = lax.dynamic_slice_in_dim(block_dest, rank * slots_in, slots_in)
    earlier = (block_seq[None, :] == seq_in[:, None]) & (all_slots[None, :] < mine[:, None])
    order = jnp.sum(earlier.astype(jnp.int32), axis=1)
    seq_ids = jnp.arange(seq_count, dtype=jnp.int32)
    length_in = jnp.sum(jnp.where(seq_ids[None, :] == seq_in[:, None], lengths[None, :], 0), axis=1)
    valid = jnp.where(dest_in >= 0, jnp.minimum(block_len, length_in - block_len * order), 0)
    at = plane * TOK + jnp.arange(TOK, dtype=jnp.int32)
    live = (at[None, :] < valid[:, None]).astype(F32).reshape(tokens, 1)
    owner_in = jnp.where(dest_in >= 0, dest_in // OWN_CAP, -1)
    owner_of = jnp.broadcast_to(owner_in[:, None], (slots_in, TOK)).reshape(1, tokens)
    route = (jnp.arange(owners, dtype=jnp.int32)[:, None] == owner_of).astype(F32)

    sent = score(where, acts, *pieces, live, route)
    got = exchange(sent, ("y", "x", "core"))

    targets = rank * OWN_CAP + jnp.arange(OWN_CAP, dtype=jnp.int32)
    source = jnp.sum(jnp.where(block_dest[None, :] == targets[:, None], all_slots[None, :], 0), axis=1)
    pick = ((source // slots_in)[:, None] == jnp.arange(owners, dtype=jnp.int32)[None, :]).astype(F32)
    member = (block_seq[:, None] == seq_ids[None, :]).astype(F32)

    owned = jnp.dot(pick, got[:, 0, :], precision=lax.Precision.HIGHEST)
    sums = got[:, 1, :].reshape(owners, 8, TOK)[:, :, :slots_in].swapaxes(0, 1).reshape(8, owners * slots_in)
    totals = jnp.dot(sums, member, precision=lax.Precision.HIGHEST)
    final = jnp.concatenate([owned, totals.reshape(-1, 128)], axis=0)
    final = exchange(jnp.broadcast_to(final[None], (PLANES, *final.shape)), "mp")
    token_rewards = (
        final[:, :OWN_CAP].reshape(PLANES, OWN_CAP, 8, TOK).transpose(1, 2, 0, 3).reshape(OWN_CAP, 8, block_len)
    )
    totals = final[:, OWN_CAP:].reshape(PLANES, 8, seq_count)
    return token_rewards, finish(totals, lengths, rank, seq_local).reshape(seq_local)


def solution(mesh):
    dp = ("y", "x", "core")
    grid = Mesh(mesh.devices.reshape(8, 4, 2, PLANES), (*dp, "mp"))

    return jax.shard_map(
        local,
        mesh=grid,
        in_specs=(
            P(dp, None, "mp"),
            P(dp, None, "mp"),
            P(None, "mp"),
            P("mp"),
            P("mp", None),
            P(),
            P(),
            P(),
        ),
        out_specs=(P(dp, None, None), P(dp)),
        check_vma=False,
    )
```

```python
import jax
import jax.numpy as jnp
from jax import lax
from jax.experimental import pallas as pl
from jax.experimental.pallas import tpu as pltpu
from jax.sharding import Mesh
from jax.sharding import PartitionSpec as P

OWN_CAP = 10
NORM_EPS = 1e-05
STAT_EPS = 1e-06
F32 = jnp.float32
BF16 = jnp.bfloat16
PLANES = 8
TOK = 16


def exchange(value, axis):
    return lax.all_to_all(value, axis, split_axis=0, concat_axis=0, tiled=True)


def shift(value, axis, step):
    size = lax.axis_size(axis)
    return lax.ppermute(value, axis, [(s, (s + step) % size) for s in range(size)])


def swap(value, axis):
    size = lax.axis_size(axis)
    return lax.ppermute(value, axis, [(s, s ^ 1) for s in range(size)])


REACH = tuple(
    tuple(((4, 1, 7, 6) if kind < 4 else (0, 2, 3, 5))[(kind + part) % 4] for part in range(4))
    for kind in range(PLANES)
)


def from_plane(value, part):
    pairs = []
    for y in range(8):
        for x in range(4):
            step = REACH[(y % 2) * 4 + x][part]
            for core in range(2):
                base = ((y * 4 + x) * 2 + core) * PLANES
                pairs += [(base + (z + step) % PLANES, base + z) for z in range(PLANES)]
    return lax.ppermute(value, ("y", "x", "core", "mp"), pairs)


def thirds(value):
    high = value.astype(BF16)
    left = value - high.astype(F32)
    mid = left.astype(BF16)
    return high, mid, (left - mid.astype(F32)).astype(BF16)


def score_kernel(
    where_ref, acts_ref, *refs,
):
    pieces = refs[:16]
    live_ref, route_ref, out_ref, a_ref, w_ref, proj_ref, resid_ref, inv_ref, sem = refs[16:]
    tokens = live_ref.shape[0]
    shard = acts_ref.shape[2]
    core = where_ref[32]
    def fetch(side, s, p):
        target = w_ref.at[side, where_ref[8 * p + s], pl.ds(p * shard, shard)]
        return pltpu.make_async_copy(pieces[2 * s + side].at[p], target, sem.at[side, s, p])

    for side in range(2):
        for s in range(8):
            for p in range(4):
                fetch(side, s, p).start()
    for p in range(4):
        a_ref[0, :, p * shard : (p + 1) * shard] = acts_ref[2 * p + core, 0:tokens, :]
        a_ref[1, :, p * shard : (p + 1) * shard] = acts_ref[2 * p + 1 - core, 0:tokens, :]
    head_rows = jnp.concatenate([acts_ref[j, 2 * tokens :, :] for j in range(PLANES)], axis=1)
    for side in range(2):
        for s in range(8):
            for p in range(4):
                fetch(side, s, p).wait()
        for j in range(PLANES):
            part = jnp.dot(a_ref[side], w_ref[side, j], preferred_element_type=F32)
            if side == 0:
                proj_ref[j] = part
            else:
                proj_ref[j] += part
    step = 16
    for row in range(0, tokens, step):
        total = jnp.zeros((step, shard), F32)
        for j in range(PLANES):
            hidden = acts_ref[j, tokens + row : tokens + row + step, :].astype(F32)
            resid = (hidden + proj_ref[j, row : row + step, :]).astype(BF16)
            resid_ref[row : row + step, j * shard : (j + 1) * shard] = resid
            value = resid.astype(F32)
            total = total + value * value
        mean_sq = jnp.sum(total, axis=1, keepdims=True) / float(PLANES * shard)
        inv_ref[row : row + step, :] = jnp.broadcast_to(lax.rsqrt(mean_sq + NORM_EPS), (step, 128))
    heads = lax.dot_general(
        resid_ref[...], head_rows, (((1,), (1,)), ((), ())), preferred_element_type=F32
    )
    k = lax.broadcasted_iota(jnp.int32, (48, 128), 0)
    lane = lax.broadcasted_iota(jnp.int32, (48, 128), 1)
    spread_heads = (k % 8 == lane // TOK).astype(BF16)
    wide = jnp.dot(jnp.concatenate(thirds(heads), axis=1), spread_heads, preferred_element_type=F32)
    wide = wide * (inv_ref[...] * live_ref[...])
    row = lax.broadcasted_iota(jnp.int32, (tokens, 128), 0)
    col = lax.broadcasted_iota(jnp.int32, (tokens, 128), 1)
    by_token = jnp.where(row % TOK == col % TOK, wide, 0.0)
    by_slot = jnp.where(row // TOK == col % TOK, wide, 0.0)
    routed = jnp.dot(
        route_ref[...], jnp.concatenate(thirds(by_token), axis=1), preferred_element_type=F32
    )
    out_ref[:, 0, :] = routed[:, 0:128] + routed[:, 128:256] + routed[:, 256:384]
    out_ref[:, 1, :] = jnp.broadcast_to(
        jnp.sum(by_slot, axis=0, keepdims=True), (out_ref.shape[0], 128)
    )


def in_vmem(value):
    return pltpu.with_memory_space_constraint(value, pltpu.VMEM)


def score(where, acts, pieces, live, route):
    owners, tokens = route.shape
    shard = acts.shape[2]
    vmem = pl.BlockSpec(memory_space=pltpu.VMEM)
    return pl.pallas_call(
        score_kernel,
        out_shape=jax.ShapeDtypeStruct((owners, 2, 128), F32),
        in_specs=[
            pl.BlockSpec(memory_space=pltpu.SMEM),
            vmem,
            *[pl.BlockSpec(memory_space=pl.ANY)] * 16,
            vmem,
            vmem,
        ],
        out_specs=vmem,
        scratch_shapes=[
            pltpu.VMEM((2, tokens, 4 * shard), BF16),
            pltpu.VMEM((2, PLANES, 4 * shard, shard), BF16),
            pltpu.VMEM((PLANES, tokens, shard), F32),
            pltpu.VMEM((tokens, PLANES * shard), BF16),
            pltpu.VMEM((tokens, 128), F32),
            pltpu.SemaphoreType.DMA((2, 8, 4)),
        ],
        compiler_params=pltpu.CompilerParams(vmem_limit_bytes=24 * 2**20),
        name="score",
    )(where, in_vmem(acts), *[pltpu.with_memory_space_constraint(v, pltpu.HBM) for v in pieces], live, route)


def finish_kernel(totals_ref, lengths_ref, rank_ref, out_ref):
    totals = totals_ref[0]
    for p in range(1, PLANES):
        totals = totals + totals_ref[p]
    scores = totals / lengths_ref[...].astype(F32)
    count = float(scores.shape[1])
    worst = jnp.min(scores, axis=0, keepdims=True)
    head_mean = jnp.mean(scores, axis=0, keepdims=True)
    spread = jnp.mean((scores - head_mean) ** 2, axis=0, keepdims=True)
    penalty_scale = jnp.sum(spread, axis=1, keepdims=True) / count + STAT_EPS
    conservative = worst - spread / penalty_scale
    centre = jnp.sum(conservative, axis=1, keepdims=True) / count
    off = conservative - centre
    variance = jnp.sum(off * off, axis=1, keepdims=True) / count
    advantages = off / jnp.sqrt(variance + STAT_EPS)
    size = out_ref.shape[0]
    at = lax.broadcasted_iota(jnp.int32, (size, scores.shape[1]), 1)
    row = lax.broadcasted_iota(jnp.int32, (size, scores.shape[1]), 0)
    mine = jnp.where(at == row + rank_ref[0] * size, advantages, 0.0)
    out_ref[...] = jnp.sum(mine, axis=1, keepdims=True)


def finish(totals, lengths, rank, size):
    vmem = pl.BlockSpec(memory_space=pltpu.VMEM)
    return pl.pallas_call(
        finish_kernel,
        out_shape=jax.ShapeDtypeStruct((size, 1), F32),
        in_specs=[vmem, vmem, pl.BlockSpec(memory_space=pltpu.SMEM)],
        out_specs=vmem,
        compiler_params=pltpu.CompilerParams(vmem_limit_bytes=8 * 2**20),
        name="finish",
    )(in_vmem(totals), lengths, rank[None])


def local(hidden, attn_out, out_proj, norm_gain, reward_proj, block_seq, block_dest, lengths):
    y, x, core, plane = (lax.axis_index(n) for n in ("y", "x", "core", "mp"))
    rank = (y * lax.axis_size("x") + x) * 2 + core
    owners = 64
    slots_in, block_len, shard = hidden.shape
    seq_count = lengths.shape[0]
    seq_local = seq_count // owners
    tokens = slots_in * TOK

    parity = y % 2
    blocks = out_proj.reshape(4, 2, shard, shard)
    parts = []
    for p in range(4):
        block = lax.dynamic_index_in_dim(blocks[p], core, 0, keepdims=False)
        parts.append(from_plane(block, p))
    first = jnp.stack(parts)

    weighted = (norm_gain[:, None] * reward_proj).T
    high = lax.reduce_precision(weighted, 8, 7)
    low = weighted - high
    head_rows = jnp.concatenate([high.astype(BF16), low.astype(BF16)], axis=0)
    sliced = [
        v.reshape(slots_in, PLANES, TOK, shard).swapaxes(0, 1).reshape(PLANES, tokens, shard)
        for v in (attn_out, hidden)
    ]
    acts = jnp.concatenate([*sliced, jnp.broadcast_to(head_rows[None], (PLANES, *head_rows.shape))], axis=1)
    acts = exchange(acts, "mp")

    second = swap(first, "y")
    left0 = shift(first, "x", 1)
    right0 = shift(first, "x", -1)
    left1 = shift(second, "x", 1)
    right1 = shift(second, "x", -1)
    far0 = shift(left0, "x", 1)
    far1 = shift(right1, "x", -1)
    held = {
        "c0": first, "c1": second, "cl0": left0, "cr0": right0,
        "cl1": left1, "cr1": right1, "cf0": far0, "cf1": far1,
    }
    pieces = []
    for own in held.values():
        pieces += [own, swap(own, "core")]
    slot = jnp.arange(8, dtype=jnp.int32)
    odd = ((slot == 1) | (slot == 4) | (slot == 5) | (slot == 7)).astype(jnp.int32)
    away = jnp.where(slot < 2, 0, jnp.where(slot > 5, 2, 3 - 2 * (slot % 2)))
    kind = (parity ^ odd) * 4 + (x + away) % 4
    turn = (kind[None, :] + jnp.arange(4, dtype=jnp.int32)[:, None]) % 4
    low_kind = jnp.where(turn == 0, 4, jnp.where(turn == 1, 1, 9 - turn))
    high_kind = jnp.where(turn == 0, 0, jnp.where(turn == 3, 5, turn + 1))
    reach = jnp.where(kind[None, :] < 4, low_kind, high_kind)
    where = jnp.concatenate([((plane + reach) % PLANES).reshape(32), core[None]]).astype(jnp.int32)

    all_slots = jnp.arange(block_seq.shape[0], dtype=jnp.int32)
    mine = rank * slots_in + jnp.arange(slots_in, dtype=jnp.int32)
    seq_in = lax.dynamic_slice_in_dim(block_seq, rank * slots_in, slots_in)
    dest_in = lax.dynamic_slice_in_dim(block_dest, rank * slots_in, slots_in)
    earlier = (block_seq[None, :] == seq_in[:, None]) & (all_slots[None, :] < mine[:, None])
    order = jnp.sum(earlier.astype(jnp.int32), axis=1)
    seq_ids = jnp.arange(seq_count, dtype=jnp.int32)
    length_in = jnp.sum(jnp.where(seq_ids[None, :] == seq_in[:, None], lengths[None, :], 0), axis=1)
    valid = jnp.where(dest_in >= 0, jnp.minimum(block_len, length_in - block_len * order), 0)
    at = plane * TOK + jnp.arange(TOK, dtype=jnp.int32)
    live = (at[None, :] < valid[:, None]).astype(F32).reshape(tokens, 1)
    live = jnp.broadcast_to(live, (tokens, 128))
    owner_in = jnp.where(dest_in >= 0, dest_in // OWN_CAP, -1)
    owner_of = jnp.broadcast_to(owner_in[:, None], (slots_in, TOK)).reshape(1, tokens)
    route = (jnp.arange(owners, dtype=jnp.int32)[:, None] == owner_of).astype(BF16)

    targets = rank * OWN_CAP + jnp.arange(OWN_CAP, dtype=jnp.int32)
    source = jnp.sum(jnp.where(block_dest[None, :] == targets[:, None], all_slots[None, :], 0), axis=1)
    source, tall, wide, where = lax.optimization_barrier(
        (source // slots_in, block_seq, lengths[None, :], where)
    )
    sent = score(where, acts, pieces, live, route)
    got = exchange(sent, ("y", "x", "core"))

    pick = (source[:, None] == jnp.arange(owners, dtype=jnp.int32)[None, :]).astype(F32)
    member = (tall[:, None] == seq_ids[None, :]).astype(F32)

    owned = jnp.dot(pick, got[:, 0, :], precision=lax.Precision.HIGHEST)
    sums = got[:, 1, :].reshape(owners, 8, TOK)[:, :, :slots_in].swapaxes(0, 1).reshape(8, owners * slots_in)
    totals = jnp.dot(sums, member, precision=lax.Precision.HIGHEST)
    final = jnp.concatenate([owned, totals.reshape(-1, 128)], axis=0)
    final = exchange(jnp.broadcast_to(final[None], (PLANES, *final.shape)), "mp")
    token_rewards = (
        final[:, :OWN_CAP].reshape(PLANES, OWN_CAP, 8, TOK).transpose(1, 2, 0, 3).reshape(OWN_CAP, 8, block_len)
    )
    totals = final[:, OWN_CAP:].reshape(PLANES, 8, seq_count)
    return token_rewards, finish(totals, wide, rank, seq_local).reshape(seq_local)


def solution(mesh):
    dp = ("y", "x", "core")
    grid = Mesh(mesh.devices.reshape(8, 4, 2, PLANES), (*dp, "mp"))

    return jax.shard_map(
        local,
        mesh=grid,
        in_specs=(
            P(dp, None, "mp"),
            P(dp, None, "mp"),
            P(None, "mp"),
            P("mp"),
            P("mp", None),
            P(),
            P(),
            P(),
        ),
        out_specs=(P(dp, None, None), P(dp)),
        check_vma=False,
    )
```

```python
import jax
import jax.numpy as jnp
from jax import lax
from jax.experimental import pallas as pl
from jax.experimental.pallas import tpu as pltpu
from jax.sharding import Mesh
from jax.sharding import PartitionSpec as P

OWN_CAP = 10
NORM_EPS = 1e-05
STAT_EPS = 1e-06
F32 = jnp.float32
BF16 = jnp.bfloat16
PLANES = 8
TOK = 16


def exchange(value, axis):
    return lax.all_to_all(value, axis, split_axis=0, concat_axis=0, tiled=True)


def shift(value, axis, step):
    size = lax.axis_size(axis)
    return lax.ppermute(value, axis, [(s, (s + step) % size) for s in range(size)])


def swap_odd(value, axis):
    size = lax.axis_size(axis)
    return lax.ppermute(value, axis, [(s, (s + 2 * (s % 2) - 1) % size) for s in range(size)])


def swap(value, axis):
    size = lax.axis_size(axis)
    return lax.ppermute(value, axis, [(s, s ^ 1) for s in range(size)])


REACH = tuple(
    tuple(((4, 1, 7, 6) if kind < 4 else (0, 2, 3, 5))[(kind + part) % 4] for part in range(4))
    for kind in range(PLANES)
)


def from_plane(value, part):
    pairs = []
    for y in range(8):
        for x in range(4):
            step = REACH[(y % 2) * 4 + x][part]
            for core in range(2):
                base = ((y * 4 + x) * 2 + core) * PLANES
                pairs += [(base + (z + step) % PLANES, base + z) for z in range(PLANES)]
    return lax.ppermute(value, ("y", "x", "core", "mp"), pairs)


def thirds(value):
    high = value.astype(BF16)
    left = value - high.astype(F32)
    mid = left.astype(BF16)
    return high, mid, (left - mid.astype(F32)).astype(BF16)


def score_kernel(
    where_ref, acts_ref, *refs,
):
    pieces = refs[:16]
    live_ref, route_ref, out_ref, a_ref, w_ref, proj_ref, resid_ref, inv_ref, sem = refs[16:]
    tokens = live_ref.shape[0]
    shard = acts_ref.shape[2]
    core = where_ref[32]
    def fetch(side, s, p):
        target = w_ref.at[side, where_ref[8 * p + s], pl.ds(p * shard, shard)]
        return pltpu.make_async_copy(pieces[2 * s + side].at[p], target, sem.at[side, s, p])

    for side in range(2):
        for s in range(8):
            for p in range(4):
                fetch(side, s, p).start()
    for p in range(4):
        a_ref[0, :, p * shard : (p + 1) * shard] = acts_ref[2 * p + core, 0:tokens, :]
        a_ref[1, :, p * shard : (p + 1) * shard] = acts_ref[2 * p + 1 - core, 0:tokens, :]
    head_rows = jnp.concatenate([acts_ref[j, 2 * tokens :, :] for j in range(PLANES)], axis=1)
    for side in range(2):
        for s in range(8):
            for p in range(4):
                fetch(side, s, p).wait()
        for j in range(PLANES):
            part = jnp.dot(a_ref[side], w_ref[side, j], preferred_element_type=F32)
            if side == 0:
                proj_ref[j] = part
            else:
                proj_ref[j] += part
    step = 16
    for row in range(0, tokens, step):
        total = jnp.zeros((step, shard), F32)
        for j in range(PLANES):
            hidden = acts_ref[j, tokens + row : tokens + row + step, :].astype(F32)
            resid = (hidden + proj_ref[j, row : row + step, :]).astype(BF16)
            resid_ref[row : row + step, j * shard : (j + 1) * shard] = resid
            value = resid.astype(F32)
            total = total + value * value
        mean_sq = jnp.sum(total, axis=1, keepdims=True) / float(PLANES * shard)
        inv_ref[row : row + step, :] = jnp.broadcast_to(lax.rsqrt(mean_sq + NORM_EPS), (step, 128))
    heads = lax.dot_general(
        resid_ref[...], head_rows, (((1,), (1,)), ((), ())), preferred_element_type=F32
    )
    k = lax.broadcasted_iota(jnp.int32, (48, 128), 0)
    lane = lax.broadcasted_iota(jnp.int32, (48, 128), 1)
    spread_heads = (k % 8 == lane // TOK).astype(BF16)
    wide = jnp.dot(jnp.concatenate(thirds(heads), axis=1), spread_heads, preferred_element_type=F32)
    wide = wide * (inv_ref[...] * live_ref[...])
    row = lax.broadcasted_iota(jnp.int32, (tokens, 128), 0)
    col = lax.broadcasted_iota(jnp.int32, (tokens, 128), 1)
    by_token = jnp.where(row % TOK == col % TOK, wide, 0.0)
    by_slot = jnp.where(row // TOK == col % TOK, wide, 0.0)
    routed = jnp.dot(
        route_ref[...], jnp.concatenate(thirds(by_token), axis=1), preferred_element_type=F32
    )
    out_ref[:, 0, :] = routed[:, 0:128] + routed[:, 128:256] + routed[:, 256:384]
    out_ref[:, 1, :] = jnp.broadcast_to(
        jnp.sum(by_slot, axis=0, keepdims=True), (out_ref.shape[0], 128)
    )


def in_vmem(value):
    return pltpu.with_memory_space_constraint(value, pltpu.VMEM)


def score(where, acts, pieces, live, route):
    owners, tokens = route.shape
    shard = acts.shape[2]
    vmem = pl.BlockSpec(memory_space=pltpu.VMEM)
    return pl.pallas_call(
        score_kernel,
        out_shape=jax.ShapeDtypeStruct((owners, 2, 128), F32),
        in_specs=[
            pl.BlockSpec(memory_space=pltpu.SMEM),
            vmem,
            *[pl.BlockSpec(memory_space=pl.ANY)] * 16,
            vmem,
            vmem,
        ],
        out_specs=vmem,
        scratch_shapes=[
            pltpu.VMEM((2, tokens, 4 * shard), BF16),
            pltpu.VMEM((2, PLANES, 4 * shard, shard), BF16),
            pltpu.VMEM((PLANES, tokens, shard), F32),
            pltpu.VMEM((tokens, PLANES * shard), BF16),
            pltpu.VMEM((tokens, 128), F32),
            pltpu.SemaphoreType.DMA((2, 8, 4)),
        ],
        compiler_params=pltpu.CompilerParams(vmem_limit_bytes=24 * 2**20),
        name="score",
    )(where, in_vmem(acts), *[pltpu.with_memory_space_constraint(v, pltpu.HBM) for v in pieces], live, route)


def finish_kernel(totals_ref, lengths_ref, rank_ref, out_ref):
    totals = totals_ref[0]
    for p in range(1, PLANES):
        totals = totals + totals_ref[p]
    scores = totals / lengths_ref[...].astype(F32)
    count = float(scores.shape[1])
    worst = jnp.min(scores, axis=0, keepdims=True)
    head_mean = jnp.mean(scores, axis=0, keepdims=True)
    spread = jnp.mean((scores - head_mean) ** 2, axis=0, keepdims=True)
    penalty_scale = jnp.sum(spread, axis=1, keepdims=True) / count + STAT_EPS
    conservative = worst - spread / penalty_scale
    centre = jnp.sum(conservative, axis=1, keepdims=True) / count
    off = conservative - centre
    variance = jnp.sum(off * off, axis=1, keepdims=True) / count
    advantages = off / jnp.sqrt(variance + STAT_EPS)
    size = out_ref.shape[1]
    total = scores.shape[1]
    turned = pltpu.roll(advantages, total - rank_ref[0] * size, axis=1)
    out_ref[...] = turned[:, 0:size]


def finish(totals, lengths, rank, size):
    vmem = pl.BlockSpec(memory_space=pltpu.VMEM)
    return pl.pallas_call(
        finish_kernel,
        out_shape=jax.ShapeDtypeStruct((1, size), F32),
        in_specs=[vmem, vmem, pl.BlockSpec(memory_space=pltpu.SMEM)],
        out_specs=vmem,
        compiler_params=pltpu.CompilerParams(vmem_limit_bytes=8 * 2**20),
        name="finish",
    )(in_vmem(totals), lengths, rank[None])


def local(hidden, attn_out, out_proj, norm_gain, reward_proj, block_seq, block_dest, lengths):
    y, x, core, plane = (lax.axis_index(n) for n in ("y", "x", "core", "mp"))
    rank = (y * lax.axis_size("x") + x) * 2 + core
    owners = 64
    slots_in, block_len, shard = hidden.shape
    seq_count = lengths.shape[0]
    seq_local = seq_count // owners
    tokens = slots_in * TOK

    parity = y % 2
    blocks = out_proj.reshape(4, 2, shard, shard)
    parts = []
    for p in range(4):
        block = lax.dynamic_index_in_dim(blocks[p], core, 0, keepdims=False)
        parts.append(from_plane(block, p))
    first = jnp.stack(parts)

    weighted = (norm_gain[:, None] * reward_proj).T
    high = lax.reduce_precision(weighted, 8, 7)
    low = weighted - high
    head_rows = jnp.concatenate([high.astype(BF16), low.astype(BF16)], axis=0)
    sliced = [
        v.reshape(slots_in, PLANES, TOK, shard).swapaxes(0, 1).reshape(PLANES, tokens, shard)
        for v in (attn_out, hidden)
    ]
    acts = jnp.concatenate([*sliced, jnp.broadcast_to(head_rows[None], (PLANES, *head_rows.shape))], axis=1)
    acts = exchange(acts, "mp")

    second = swap(first, "y")
    left0 = shift(first, "x", 1)
    right0 = shift(first, "x", -1)
    left1 = swap_odd(left0, "y")
    right1 = shift(second, "x", -1)
    far0 = shift(left0, "x", 1)
    far1 = swap(far0, "y")
    held = {
        "c0": first, "c1": second, "cl0": left0, "cr0": right0,
        "cl1": left1, "cr1": right1, "cf0": far0, "cf1": far1,
    }
    pieces = []
    for own in held.values():
        pieces += [own, swap(own, "core")]
    slot = jnp.arange(8, dtype=jnp.int32)
    odd = ((slot == 1) | (slot == 4) | (slot == 5) | (slot == 7)).astype(jnp.int32)
    away = jnp.where(slot < 2, 0, jnp.where(slot > 5, 2, 3 - 2 * (slot % 2)))
    kind = (parity ^ odd) * 4 + (x + away) % 4
    turn = (kind[None, :] + jnp.arange(4, dtype=jnp.int32)[:, None]) % 4
    low_kind = jnp.where(turn == 0, 4, jnp.where(turn == 1, 1, 9 - turn))
    high_kind = jnp.where(turn == 0, 0, jnp.where(turn == 3, 5, turn + 1))
    reach = jnp.where(kind[None, :] < 4, low_kind, high_kind)
    where = jnp.concatenate([((plane + reach) % PLANES).reshape(32), core[None]]).astype(jnp.int32)

    all_slots = jnp.arange(block_seq.shape[0], dtype=jnp.int32)
    mine = rank * slots_in + jnp.arange(slots_in, dtype=jnp.int32)
    seq_in = lax.dynamic_slice_in_dim(block_seq, rank * slots_in, slots_in)
    dest_in = lax.dynamic_slice_in_dim(block_dest, rank * slots_in, slots_in)
    earlier = (block_seq[None, :] == seq_in[:, None]) & (all_slots[None, :] < mine[:, None])
    order = jnp.sum(earlier.astype(jnp.int32), axis=1)
    seq_ids = jnp.arange(seq_count, dtype=jnp.int32)
    length_in = jnp.sum(jnp.where(seq_ids[None, :] == seq_in[:, None], lengths[None, :], 0), axis=1)
    valid = jnp.where(dest_in >= 0, jnp.minimum(block_len, length_in - block_len * order), 0)
    at = plane * TOK + jnp.arange(TOK, dtype=jnp.int32)
    live = (at[None, :] < valid[:, None]).astype(F32).reshape(tokens, 1)
    live = jnp.broadcast_to(live, (tokens, 128))
    owner_in = jnp.where(dest_in >= 0, dest_in // OWN_CAP, -1)
    owner_of = jnp.broadcast_to(owner_in[:, None], (slots_in, TOK)).reshape(1, tokens)
    route = (jnp.arange(owners, dtype=jnp.int32)[:, None] == owner_of).astype(BF16)

    targets = rank * OWN_CAP + jnp.arange(OWN_CAP, dtype=jnp.int32)
    source = jnp.sum(jnp.where(block_dest[None, :] == targets[:, None], all_slots[None, :], 0), axis=1)
    source, tall, wide, where = lax.optimization_barrier(
        (source // slots_in, block_seq, lengths[None, :], where)
    )
    sent = score(where, acts, pieces, live, route)
    got = exchange(sent, ("y", "x", "core"))

    pick = (source[:, None] == jnp.arange(owners, dtype=jnp.int32)[None, :]).astype(F32)
    member = (tall[:, None] == seq_ids[None, :]).astype(F32)

    owned = jnp.dot(pick, got[:, 0, :], precision=lax.Precision.HIGHEST)
    sums = got[:, 1, :].reshape(owners, 8, TOK)[:, :, :slots_in].swapaxes(0, 1).reshape(8, owners * slots_in)
    totals = jnp.dot(sums, member, precision=lax.Precision.HIGHEST)
    final = jnp.concatenate([owned, totals.reshape(-1, 128)], axis=0)
    final = exchange(jnp.broadcast_to(final[None], (PLANES, *final.shape)), "mp")
    token_rewards = (
        final[:, :OWN_CAP].reshape(PLANES, OWN_CAP, 8, TOK).transpose(1, 2, 0, 3).reshape(OWN_CAP, 8, block_len)
    )
    totals = final[:, OWN_CAP:].reshape(PLANES, 8, seq_count)
    return token_rewards, finish(totals, wide, rank, seq_local).reshape(seq_local)


def solution(mesh):
    dp = ("y", "x", "core")
    grid = Mesh(mesh.devices.reshape(8, 4, 2, PLANES), (*dp, "mp"))

    return jax.shard_map(
        local,
        mesh=grid,
        in_specs=(
            P(dp, None, "mp"),
            P(dp, None, "mp"),
            P(None, "mp"),
            P("mp"),
            P("mp", None),
            P(),
            P(),
            P(),
        ),
        out_specs=(P(dp, None, None), P(dp)),
        check_vma=False,
    )
```

```python
import jax
import jax.numpy as jnp
from jax import lax
from jax.experimental import pallas as pl
from jax.experimental.pallas import tpu as pltpu
from jax.sharding import Mesh
from jax.sharding import PartitionSpec as P

OWN_CAP = 10
NORM_EPS = 1e-05
STAT_EPS = 1e-06
F32 = jnp.float32
BF16 = jnp.bfloat16
PLANES = 8
TOK = 16

CHUNKS = ((0, 0, 2), (0, 2, 2), (1, 0, 2), (1, 2, 1), (1, 3, 1))


def exchange(value, axis):
    return lax.all_to_all(value, axis, split_axis=0, concat_axis=0, tiled=True)


def shift(value, axis, step):
    size = lax.axis_size(axis)
    return lax.ppermute(value, axis, [(s, (s + step) % size) for s in range(size)])


def swap_odd(value, axis):
    size = lax.axis_size(axis)
    return lax.ppermute(value, axis, [(s, (s + 2 * (s % 2) - 1) % size) for s in range(size)])


def swap(value, axis):
    size = lax.axis_size(axis)
    return lax.ppermute(value, axis, [(s, s ^ 1) for s in range(size)])


REACH = tuple(
    tuple(((4, 1, 7, 6) if kind < 4 else (0, 2, 3, 5))[(kind + part) % 4] for part in range(4))
    for kind in range(PLANES)
)


def from_plane(value, part):
    pairs = []
    for y in range(8):
        for x in range(4):
            step = REACH[(y % 2) * 4 + x][part]
            for core in range(2):
                base = ((y * 4 + x) * 2 + core) * PLANES
                pairs += [(base + (z + step) % PLANES, base + z) for z in range(PLANES)]
    return lax.ppermute(value, ("y", "x", "core", "mp"), pairs)


def thirds(value):
    high = value.astype(BF16)
    left = value - high.astype(F32)
    mid = left.astype(BF16)
    return high, mid, (left - mid.astype(F32)).astype(BF16)


def score_kernel(
    where_ref, acts_ref, *refs,
):
    pieces = refs[:16]
    live_ref, route_ref, out_ref, a_ref, w_ref, proj_ref, resid_ref, inv_ref, sem = refs[16:]
    tokens = live_ref.shape[0]
    shard = acts_ref.shape[2]
    core = where_ref[32]
    def fetch(side, s, p):
        target = w_ref.at[side, where_ref[8 * p + s], pl.ds(p * shard, shard)]
        return pltpu.make_async_copy(pieces[2 * s + side].at[p], target, sem.at[side, s, p])

    for side in range(2):
        for p in range(4):
            for s in range(8):
                fetch(side, s, p).start()
    for p in range(4):
        a_ref[0, :, p * shard : (p + 1) * shard] = acts_ref[2 * p + core, 0:tokens, :]
        a_ref[1, :, p * shard : (p + 1) * shard] = acts_ref[2 * p + 1 - core, 0:tokens, :]
    head_rows = jnp.concatenate([acts_ref[j, 2 * tokens :, :] for j in range(PLANES)], axis=1)
    for side, p, parts in CHUNKS:
        for q in range(p, p + parts):
            for s in range(8):
                fetch(side, s, q).wait()
        at = slice(p * shard, (p + parts) * shard)
        for j in range(PLANES):
            part = jnp.dot(a_ref[side, :, at], w_ref[side, j, at], preferred_element_type=F32)
            if side == 0 and p == 0:
                proj_ref[j] = part
            else:
                proj_ref[j] += part
    step = 16
    for row in range(0, tokens, step):
        total = jnp.zeros((step, shard), F32)
        for j in range(PLANES):
            hidden = acts_ref[j, tokens + row : tokens + row + step, :].astype(F32)
            resid = (hidden + proj_ref[j, row : row + step, :]).astype(BF16)
            resid_ref[row : row + step, j * shard : (j + 1) * shard] = resid
            value = resid.astype(F32)
            total = total + value * value
        mean_sq = jnp.sum(total, axis=1, keepdims=True) / float(PLANES * shard)
        inv_ref[row : row + step, :] = jnp.broadcast_to(lax.rsqrt(mean_sq + NORM_EPS), (step, 128))
    heads = lax.dot_general(
        resid_ref[...], head_rows, (((1,), (1,)), ((), ())), preferred_element_type=F32
    )
    k = lax.broadcasted_iota(jnp.int32, (48, 128), 0)
    lane = lax.broadcasted_iota(jnp.int32, (48, 128), 1)
    spread_heads = (k % 8 == lane // TOK).astype(BF16)
    wide = jnp.dot(jnp.concatenate(thirds(heads), axis=1), spread_heads, preferred_element_type=F32)
    wide = wide * (inv_ref[...] * live_ref[...])
    row = lax.broadcasted_iota(jnp.int32, (tokens, 128), 0)
    col = lax.broadcasted_iota(jnp.int32, (tokens, 128), 1)
    by_token = jnp.where(row % TOK == col % TOK, wide, 0.0)
    by_slot = jnp.where(row // TOK == col % TOK, wide, 0.0)
    routed = jnp.dot(
        route_ref[...], jnp.concatenate(thirds(by_token), axis=1), preferred_element_type=F32
    )
    out_ref[:, 0, :] = routed[:, 0:128] + routed[:, 128:256] + routed[:, 256:384]
    out_ref[:, 1, :] = jnp.broadcast_to(
        jnp.sum(by_slot, axis=0, keepdims=True), (out_ref.shape[0], 128)
    )


def in_vmem(value):
    return pltpu.with_memory_space_constraint(value, pltpu.VMEM)


def score(where, acts, pieces, live, route):
    owners, tokens = route.shape
    shard = acts.shape[2]
    vmem = pl.BlockSpec(memory_space=pltpu.VMEM)
    return pl.pallas_call(
        score_kernel,
        out_shape=jax.ShapeDtypeStruct((owners, 2, 128), F32),
        in_specs=[
            pl.BlockSpec(memory_space=pltpu.SMEM),
            vmem,
            *[pl.BlockSpec(memory_space=pl.ANY)] * 16,
            vmem,
            vmem,
        ],
        out_specs=vmem,
        scratch_shapes=[
            pltpu.VMEM((2, tokens, 4 * shard), BF16),
            pltpu.VMEM((2, PLANES, 4 * shard, shard), BF16),
            pltpu.VMEM((PLANES, tokens, shard), F32),
            pltpu.VMEM((tokens, PLANES * shard), BF16),
            pltpu.VMEM((tokens, 128), F32),
            pltpu.SemaphoreType.DMA((2, 8, 4)),
        ],
        compiler_params=pltpu.CompilerParams(vmem_limit_bytes=24 * 2**20),
        name="score",
    )(where, in_vmem(acts), *[pltpu.with_memory_space_constraint(v, pltpu.HBM) for v in pieces], live, route)


def gather_kernel(source_ref, got_ref, totals_ref, out_ref):
    owned = jnp.concatenate([got_ref[source_ref[q], 0:1, :] for q in range(OWN_CAP)], axis=0)
    groups = totals_ref.shape[1] // 128
    for p in range(PLANES):
        for g in range(groups):
            out_ref[p, 8 * g : 8 * g + 8, :] = totals_ref[:, 128 * g : 128 * g + 128]
        out_ref[p, 8 * groups : 8 * groups + OWN_CAP, :] = owned


def gather(source, got, totals):
    vmem = pl.BlockSpec(memory_space=pltpu.VMEM)
    rows = totals.shape[1] // 128 * 8 + OWN_CAP
    return pl.pallas_call(
        gather_kernel,
        out_shape=jax.ShapeDtypeStruct((PLANES, rows, 128), F32),
        in_specs=[pl.BlockSpec(memory_space=pltpu.SMEM), vmem, vmem],
        out_specs=vmem,
        compiler_params=pltpu.CompilerParams(vmem_limit_bytes=8 * 2**20),
        name="gather",
    )(source, in_vmem(got), in_vmem(totals))


def finish_kernel(final_ref, lengths_ref, rank_ref, out_ref):
    groups = lengths_ref.shape[1] // 128
    totals = final_ref[0, 0 : 8 * groups, :]
    for p in range(1, PLANES):
        totals = totals + final_ref[p, 0 : 8 * groups, :]
    totals = jnp.concatenate([totals[8 * g : 8 * g + 8, :] for g in range(groups)], axis=1)
    scores = totals / lengths_ref[...].astype(F32)
    count = float(scores.shape[1])
    worst = jnp.min(scores, axis=0, keepdims=True)
    head_mean = jnp.mean(scores, axis=0, keepdims=True)
    spread = jnp.mean((scores - head_mean) ** 2, axis=0, keepdims=True)
    penalty_scale = jnp.sum(spread, axis=1, keepdims=True) / count + STAT_EPS
    conservative = worst - spread / penalty_scale
    centre = jnp.sum(conservative, axis=1, keepdims=True) / count
    off = conservative - centre
    variance = jnp.sum(off * off, axis=1, keepdims=True) / count
    advantages = off / jnp.sqrt(variance + STAT_EPS)
    size = out_ref.shape[1]
    total = scores.shape[1]
    turned = pltpu.roll(advantages, total - rank_ref[0] * size, axis=1)
    out_ref[...] = turned[:, 0:size]


def finish(final, lengths, rank, size):
    vmem = pl.BlockSpec(memory_space=pltpu.VMEM)
    return pl.pallas_call(
        finish_kernel,
        out_shape=jax.ShapeDtypeStruct((1, size), F32),
        in_specs=[vmem, vmem, pl.BlockSpec(memory_space=pltpu.SMEM)],
        out_specs=vmem,
        compiler_params=pltpu.CompilerParams(vmem_limit_bytes=8 * 2**20),
        name="finish",
    )(in_vmem(final), lengths, rank[None])


def local(hidden, attn_out, out_proj, norm_gain, reward_proj, block_seq, block_dest, lengths):
    y, x, core, plane = (lax.axis_index(n) for n in ("y", "x", "core", "mp"))
    rank = (y * lax.axis_size("x") + x) * 2 + core
    owners = 64
    slots_in, block_len, shard = hidden.shape
    seq_count = lengths.shape[0]
    seq_local = seq_count // owners
    tokens = slots_in * TOK

    parity = y % 2
    blocks = out_proj.reshape(4, 2, shard, shard)
    parts = []
    for p in range(4):
        block = lax.dynamic_index_in_dim(blocks[p], core, 0, keepdims=False)
        parts.append(from_plane(block, p))
    first = jnp.stack(parts)

    weighted = (norm_gain[:, None] * reward_proj).T
    high = lax.reduce_precision(weighted, 8, 7)
    low = weighted - high
    head_rows = jnp.concatenate([high.astype(BF16), low.astype(BF16)], axis=0)
    sliced = [
        v.reshape(slots_in, PLANES, TOK, shard).swapaxes(0, 1).reshape(PLANES, tokens, shard)
        for v in (attn_out, hidden)
    ]
    acts = jnp.concatenate([*sliced, jnp.broadcast_to(head_rows[None], (PLANES, *head_rows.shape))], axis=1)
    acts = exchange(acts, "mp")

    second = swap(first, "y")
    left0 = shift(first, "x", 1)
    right0 = shift(first, "x", -1)
    left1 = swap_odd(left0, "y")
    right1 = shift(second, "x", -1)
    far0 = shift(left0, "x", 1)
    far1 = swap(far0, "y")
    held = {
        "c0": first, "c1": second, "cl0": left0, "cr0": right0,
        "cl1": left1, "cr1": right1, "cf0": far0, "cf1": far1,
    }
    pieces = []
    for own in held.values():
        pieces += [own, swap(own, "core")]
    slot = jnp.arange(8, dtype=jnp.int32)
    odd = ((slot == 1) | (slot == 4) | (slot == 5) | (slot == 7)).astype(jnp.int32)
    away = jnp.where(slot < 2, 0, jnp.where(slot > 5, 2, 3 - 2 * (slot % 2)))
    kind = (parity ^ odd) * 4 + (x + away) % 4
    turn = (kind[None, :] + jnp.arange(4, dtype=jnp.int32)[:, None]) % 4
    low_kind = jnp.where(turn == 0, 4, jnp.where(turn == 1, 1, 9 - turn))
    high_kind = jnp.where(turn == 0, 0, jnp.where(turn == 3, 5, turn + 1))
    reach = jnp.where(kind[None, :] < 4, low_kind, high_kind)
    where = jnp.concatenate([((plane + reach) % PLANES).reshape(32), core[None]]).astype(jnp.int32)

    all_slots = jnp.arange(block_seq.shape[0], dtype=jnp.int32)
    mine = rank * slots_in + jnp.arange(slots_in, dtype=jnp.int32)
    seq_in = lax.dynamic_slice_in_dim(block_seq, rank * slots_in, slots_in)
    dest_in = lax.dynamic_slice_in_dim(block_dest, rank * slots_in, slots_in)
    earlier = (block_seq[None, :] == seq_in[:, None]) & (all_slots[None, :] < mine[:, None])
    order = jnp.sum(earlier.astype(jnp.int32), axis=1)
    seq_ids = jnp.arange(seq_count, dtype=jnp.int32)
    length_in = jnp.sum(jnp.where(seq_ids[None, :] == seq_in[:, None], lengths[None, :], 0), axis=1)
    valid = jnp.where(dest_in >= 0, jnp.minimum(block_len, length_in - block_len * order), 0)
    at = plane * TOK + jnp.arange(TOK, dtype=jnp.int32)
    live = (at[None, :] < valid[:, None]).astype(F32).reshape(tokens, 1)
    live = jnp.broadcast_to(live, (tokens, 128))
    owner_in = jnp.where(dest_in >= 0, dest_in // OWN_CAP, -1)
    owner_of = jnp.broadcast_to(owner_in[:, None], (slots_in, TOK)).reshape(1, tokens)
    route = (jnp.arange(owners, dtype=jnp.int32)[:, None] == owner_of).astype(BF16)

    targets = rank * OWN_CAP + jnp.arange(OWN_CAP, dtype=jnp.int32)
    source = jnp.sum(jnp.where(block_dest[None, :] == targets[:, None], all_slots[None, :], 0), axis=1)
    source, tall, wide, where = lax.optimization_barrier(
        (jnp.minimum(source // slots_in, owners - 1), block_seq, lengths[None, :], where)
    )
    sent = score(where, acts, pieces, live, route)
    got = exchange(sent, ("y", "x", "core"))

    member = (tall[:, None] == seq_ids[None, :]).astype(F32)
    sums = got[:, 1, :].reshape(owners, 8, TOK)[:, :, :slots_in].swapaxes(0, 1).reshape(8, owners * slots_in)
    totals = jnp.dot(sums, member, precision=lax.Precision.HIGHEST)
    final = exchange(gather(source, got, totals), "mp")
    token_rewards = (
        final[:, -OWN_CAP:].reshape(PLANES, OWN_CAP, 8, TOK).transpose(1, 2, 0, 3).reshape(OWN_CAP, 8, block_len)
    )
    return token_rewards, finish(final, wide, rank, seq_local).reshape(seq_local)


def solution(mesh):
    dp = ("y", "x", "core")
    grid = Mesh(mesh.devices.reshape(8, 4, 2, PLANES), (*dp, "mp"))

    return jax.shard_map(
        local,
        mesh=grid,
        in_specs=(
            P(dp, None, "mp"),
            P(dp, None, "mp"),
            P(None, "mp"),
            P("mp"),
            P("mp", None),
            P(),
            P(),
            P(),
        ),
        out_specs=(P(dp, None, None), P(dp)),
        check_vma=False,
    )
```

```python
import jax
import jax.numpy as jnp
from jax import lax
from jax.experimental import pallas as pl
from jax.experimental.pallas import tpu as pltpu
from jax.sharding import Mesh
from jax.sharding import PartitionSpec as P

OWN_CAP = 10
NORM_EPS = 1e-05
STAT_EPS = 1e-06
F32 = jnp.float32
BF16 = jnp.bfloat16
PLANES = 8
TOK = 16

CHUNKS = ((0, 0, 2), (0, 2, 2), (1, 0, 2), (1, 2, 1), (1, 3, 1))


def exchange(value, axis):
    return lax.all_to_all(value, axis, split_axis=0, concat_axis=0, tiled=True)


def shift(value, axis, step):
    size = lax.axis_size(axis)
    return lax.ppermute(value, axis, [(s, (s + step) % size) for s in range(size)])


def swap_odd(value, axis):
    size = lax.axis_size(axis)
    return lax.ppermute(value, axis, [(s, (s + 2 * (s % 2) - 1) % size) for s in range(size)])


def swap(value, axis):
    size = lax.axis_size(axis)
    return lax.ppermute(value, axis, [(s, s ^ 1) for s in range(size)])


REACH = tuple(
    tuple(((4, 1, 7, 6) if kind < 4 else (0, 2, 3, 5))[(kind + part) % 4] for part in range(4))
    for kind in range(PLANES)
)


def from_plane(value, part):
    pairs = []
    for y in range(8):
        for x in range(4):
            step = REACH[(y % 2) * 4 + x][part]
            for core in range(2):
                base = ((y * 4 + x) * 2 + core) * PLANES
                pairs += [(base + (z + step) % PLANES, base + z) for z in range(PLANES)]
    return lax.ppermute(value, ("y", "x", "core", "mp"), pairs)


def thirds(value):
    high = value.astype(BF16)
    left = value - high.astype(F32)
    mid = left.astype(BF16)
    return high, mid, (left - mid.astype(F32)).astype(BF16)


def score_kernel(
    where_ref, acts_ref, *refs,
):
    pieces = refs[:16]
    live_ref, route_ref, out_ref, a_ref, w_ref, proj_ref, resid_ref, inv_ref, sem = refs[16:]
    tokens = live_ref.shape[0]
    shard = acts_ref.shape[2]
    core = where_ref[32]
    def fetch(side, s, p):
        target = w_ref.at[side, where_ref[8 * p + s], pl.ds(p * shard, shard)]
        return pltpu.make_async_copy(pieces[2 * s + side].at[p], target, sem.at[side, s, p])

    for side in range(2):
        for p in range(4):
            for s in range(8):
                fetch(side, s, p).start()
    for p in range(4):
        a_ref[0, :, p * shard : (p + 1) * shard] = acts_ref[2 * p + core, 0:tokens, :]
        a_ref[1, :, p * shard : (p + 1) * shard] = acts_ref[2 * p + 1 - core, 0:tokens, :]
    head_rows = jnp.concatenate([acts_ref[j, 2 * tokens :, :] for j in range(PLANES)], axis=1)
    for side, p, parts in CHUNKS:
        for q in range(p, p + parts):
            for s in range(8):
                fetch(side, s, q).wait()
        at = slice(p * shard, (p + parts) * shard)
        for j in range(PLANES):
            part = jnp.dot(a_ref[side, :, at], w_ref[side, j, at], preferred_element_type=F32)
            if side == 0 and p == 0:
                proj_ref[j] = part
            else:
                proj_ref[j] += part
    step = 16
    for row in range(0, tokens, step):
        total = jnp.zeros((step, shard), F32)
        for j in range(PLANES):
            hidden = acts_ref[j, tokens + row : tokens + row + step, :].astype(F32)
            resid = (hidden + proj_ref[j, row : row + step, :]).astype(BF16)
            resid_ref[row : row + step, j * shard : (j + 1) * shard] = resid
            value = resid.astype(F32)
            total = total + value * value
        mean_sq = jnp.sum(total, axis=1, keepdims=True) / float(PLANES * shard)
        inv_ref[row : row + step, :] = jnp.broadcast_to(lax.rsqrt(mean_sq + NORM_EPS), (step, 128))
    heads = lax.dot_general(
        resid_ref[...], head_rows, (((1,), (1,)), ((), ())), preferred_element_type=F32
    )
    k = lax.broadcasted_iota(jnp.int32, (48, 128), 0)
    lane = lax.broadcasted_iota(jnp.int32, (48, 128), 1)
    spread_heads = (k % 8 == lane // TOK).astype(BF16)
    wide = jnp.dot(jnp.concatenate(thirds(heads), axis=1), spread_heads, preferred_element_type=F32)
    wide = wide * (inv_ref[...] * live_ref[...])
    row = lax.broadcasted_iota(jnp.int32, (tokens, 128), 0)
    col = lax.broadcasted_iota(jnp.int32, (tokens, 128), 1)
    by_token = jnp.where(row % TOK == col % TOK, wide, 0.0)
    by_slot = jnp.where(row // TOK == col % TOK, wide, 0.0)
    routed = jnp.dot(
        route_ref[...], jnp.concatenate(thirds(by_token), axis=1), preferred_element_type=F32
    )
    out_ref[:, 0, :] = routed[:, 0:128] + routed[:, 128:256] + routed[:, 256:384]
    out_ref[:, 1, :] = jnp.broadcast_to(
        jnp.sum(by_slot, axis=0, keepdims=True), (out_ref.shape[0], 128)
    )


def in_vmem(value):
    return pltpu.with_memory_space_constraint(value, pltpu.VMEM)


def score(where, acts, pieces, live, route):
    owners, tokens = route.shape
    shard = acts.shape[2]
    vmem = pl.BlockSpec(memory_space=pltpu.VMEM)
    return pl.pallas_call(
        score_kernel,
        out_shape=jax.ShapeDtypeStruct((owners, 2, 128), F32),
        in_specs=[
            pl.BlockSpec(memory_space=pltpu.SMEM),
            vmem,
            *[pl.BlockSpec(memory_space=pl.ANY)] * 16,
            vmem,
            vmem,
        ],
        out_specs=vmem,
        scratch_shapes=[
            pltpu.VMEM((2, tokens, 4 * shard), BF16),
            pltpu.VMEM((2, PLANES, 4 * shard, shard), BF16),
            pltpu.VMEM((PLANES, tokens, shard), F32),
            pltpu.VMEM((tokens, PLANES * shard), BF16),
            pltpu.VMEM((tokens, 128), F32),
            pltpu.SemaphoreType.DMA((2, 8, 4)),
        ],
        compiler_params=pltpu.CompilerParams(vmem_limit_bytes=24 * 2**20),
        name="score",
    )(where, in_vmem(acts), *[pltpu.with_memory_space_constraint(v, pltpu.HBM) for v in pieces], live, route)


def finish_kernel(totals_ref, lengths_ref, rank_ref, out_ref):
    totals = totals_ref[0]
    for p in range(1, PLANES):
        totals = totals + totals_ref[p]
    scores = totals / lengths_ref[...].astype(F32)
    count = float(scores.shape[1])
    worst = jnp.min(scores, axis=0, keepdims=True)
    head_mean = jnp.mean(scores, axis=0, keepdims=True)
    spread = jnp.mean((scores - head_mean) ** 2, axis=0, keepdims=True)
    penalty_scale = jnp.sum(spread, axis=1, keepdims=True) / count + STAT_EPS
    conservative = worst - spread / penalty_scale
    centre = jnp.sum(conservative, axis=1, keepdims=True) / count
    off = conservative - centre
    variance = jnp.sum(off * off, axis=1, keepdims=True) / count
    advantages = off / jnp.sqrt(variance + STAT_EPS)
    size = out_ref.shape[1]
    total = scores.shape[1]
    turned = pltpu.roll(advantages, total - rank_ref[0] * size, axis=1)
    out_ref[...] = turned[:, 0:size]


def finish(totals, lengths, rank, size):
    vmem = pl.BlockSpec(memory_space=pltpu.VMEM)
    return pl.pallas_call(
        finish_kernel,
        out_shape=jax.ShapeDtypeStruct((1, size), F32),
        in_specs=[vmem, vmem, pl.BlockSpec(memory_space=pltpu.SMEM)],
        out_specs=vmem,
        compiler_params=pltpu.CompilerParams(vmem_limit_bytes=8 * 2**20),
        name="finish",
    )(in_vmem(totals), lengths, rank[None])


def local(hidden, attn_out, out_proj, norm_gain, reward_proj, block_seq, block_dest, lengths):
    y, x, core, plane = (lax.axis_index(n) for n in ("y", "x", "core", "mp"))
    rank = (y * lax.axis_size("x") + x) * 2 + core
    owners = 64
    slots_in, block_len, shard = hidden.shape
    seq_count = lengths.shape[0]
    seq_local = seq_count // owners
    tokens = slots_in * TOK

    parity = y % 2
    blocks = out_proj.reshape(4, 2, shard, shard)
    parts = []
    for p in range(4):
        block = lax.dynamic_index_in_dim(blocks[p], core, 0, keepdims=False)
        parts.append(from_plane(block, p))
    first = jnp.stack(parts)

    weighted = (norm_gain[:, None] * reward_proj).T
    high = lax.reduce_precision(weighted, 8, 7)
    low = weighted - high
    head_rows = jnp.concatenate([high.astype(BF16), low.astype(BF16)], axis=0)
    sliced = [
        v.reshape(slots_in, PLANES, TOK, shard).swapaxes(0, 1).reshape(PLANES, tokens, shard)
        for v in (attn_out, hidden)
    ]
    acts = jnp.concatenate([*sliced, jnp.broadcast_to(head_rows[None], (PLANES, *head_rows.shape))], axis=1)
    acts = exchange(acts, "mp")

    second = swap(first, "y")
    left0 = shift(first, "x", 1)
    right0 = shift(first, "x", -1)
    left1 = swap_odd(left0, "y")
    right1 = shift(second, "x", -1)
    far0 = shift(left0, "x", 1)
    far1 = swap(far0, "y")
    held = {
        "c0": first, "c1": second, "cl0": left0, "cr0": right0,
        "cl1": left1, "cr1": right1, "cf0": far0, "cf1": far1,
    }
    pieces = []
    for own in held.values():
        pieces += [own, swap(own, "core")]
    slot = jnp.arange(8, dtype=jnp.int32)
    odd = ((slot == 1) | (slot == 4) | (slot == 5) | (slot == 7)).astype(jnp.int32)
    away = jnp.where(slot < 2, 0, jnp.where(slot > 5, 2, 3 - 2 * (slot % 2)))
    kind = (parity ^ odd) * 4 + (x + away) % 4
    turn = (kind[None, :] + jnp.arange(4, dtype=jnp.int32)[:, None]) % 4
    low_kind = jnp.where(turn == 0, 4, jnp.where(turn == 1, 1, 9 - turn))
    high_kind = jnp.where(turn == 0, 0, jnp.where(turn == 3, 5, turn + 1))
    reach = jnp.where(kind[None, :] < 4, low_kind, high_kind)
    where = jnp.concatenate([((plane + reach) % PLANES).reshape(32), core[None]]).astype(jnp.int32)

    all_slots = jnp.arange(block_seq.shape[0], dtype=jnp.int32)
    mine = rank * slots_in + jnp.arange(slots_in, dtype=jnp.int32)
    seq_in = lax.dynamic_slice_in_dim(block_seq, rank * slots_in, slots_in)
    dest_in = lax.dynamic_slice_in_dim(block_dest, rank * slots_in, slots_in)
    earlier = (block_seq[None, :] == seq_in[:, None]) & (all_slots[None, :] < mine[:, None])
    order = jnp.sum(earlier.astype(jnp.int32), axis=1)
    seq_ids = jnp.arange(seq_count, dtype=jnp.int32)
    length_in = jnp.sum(jnp.where(seq_ids[None, :] == seq_in[:, None], lengths[None, :], 0), axis=1)
    valid = jnp.where(dest_in >= 0, jnp.minimum(block_len, length_in - block_len * order), 0)
    at = plane * TOK + jnp.arange(TOK, dtype=jnp.int32)
    live = (at[None, :] < valid[:, None]).astype(F32).reshape(tokens, 1)
    live = jnp.broadcast_to(live, (tokens, 128))
    owner_in = jnp.where(dest_in >= 0, dest_in // OWN_CAP, -1)
    owner_of = jnp.broadcast_to(owner_in[:, None], (slots_in, TOK)).reshape(1, tokens)
    route = (jnp.arange(owners, dtype=jnp.int32)[:, None] == owner_of).astype(BF16)

    targets = rank * OWN_CAP + jnp.arange(OWN_CAP, dtype=jnp.int32)
    source = jnp.sum(jnp.where(block_dest[None, :] == targets[:, None], all_slots[None, :], 0), axis=1)
    source, tall, wide, where = lax.optimization_barrier(
        (source // slots_in, block_seq, lengths[None, :], where)
    )
    sent = score(where, acts, pieces, live, route)
    got = exchange(sent, ("y", "x", "core"))

    pick = (source[:, None] == jnp.arange(owners, dtype=jnp.int32)[None, :]).astype(F32)
    member = (tall[:, None] == seq_ids[None, :]).astype(F32)

    owned = jnp.dot(pick, got[:, 0, :], precision=lax.Precision.HIGHEST)
    sums = got[:, 1, :].reshape(owners, 8, TOK)[:, :, :slots_in].swapaxes(0, 1).reshape(8, owners * slots_in)
    totals = jnp.dot(sums, member, precision=lax.Precision.HIGHEST)
    final = jnp.concatenate([owned, totals.reshape(-1, 128)], axis=0)
    final = exchange(jnp.broadcast_to(final[None], (PLANES, *final.shape)), "mp")
    token_rewards = (
        final[:, :OWN_CAP].reshape(PLANES, OWN_CAP, 8, TOK).transpose(1, 2, 0, 3).reshape(OWN_CAP, 8, block_len)
    )
    totals = final[:, OWN_CAP:].reshape(PLANES, 8, seq_count)
    return token_rewards, finish(totals, wide, rank, seq_local).reshape(seq_local)


def solution(mesh):
    dp = ("y", "x", "core")
    grid = Mesh(mesh.devices.reshape(8, 4, 2, PLANES), (*dp, "mp"))

    return jax.shard_map(
        local,
        mesh=grid,
        in_specs=(
            P(dp, None, "mp"),
            P(dp, None, "mp"),
            P(None, "mp"),
            P("mp"),
            P("mp", None),
            P(),
            P(),
            P(),
        ),
        out_specs=(P(dp, None, None), P(dp)),
        check_vma=False,
    )
```
